256 devices in a mesh: grp: 8 (over x, core), mem: 32 (over y, z).
Axes of the slice: x: 4, y: 4, z: 8, core: 2. Of those that a mesh axis runs over, the one named last changes fastest.
Arguments:
- layer_input: bfloat16 [524288, 128], P(('grp', 'mem')), may hold values from -6 to 6
- history: bfloat16 [524288, 128], P(('grp', 'mem')), may hold values from -6 to 6
- adjacency: bfloat16 [8, 32, 16, 8, 128, 128], P('grp', 'mem'), may hold values from 0 to 0.049804688
- tile_source: int32 [8, 32, 16, 8], P('grp', 'mem'), may hold values from 0 to 63, as said below
- counts: int32 [8, 32, 16], P('grp', 'mem'), may hold values from 3 to 8, as said below
- requests: int32 [8, 32, 32, 1], P('grp', 'mem'), may hold values from 0 to 15
- send_ids: int32 [8, 32, 8, 2], P('grp', 'mem'), may hold values from 0 to 15
- weight: bfloat16 [128, 128], replicated, may hold values from -0.5 to 0.5
- layer_bias: float32 [128], replicated, may hold values from -3 to 3
- cotangent: bfloat16 [524288, 128], P(('grp', 'mem')), may hold values from -6 to 6
Outputs:
- layer_output: bfloat16 [524288, 128], P(('grp', 'mem'))
- input_grad: bfloat16 [524288, 128], P(('grp', 'mem'))
- weight_grad: float32 [128, 128], replicated
- bias_grad: float32 [128], replicated
The draws below stay inside these ranges and needn't reach their ends.
Inputs may be any that keep to these rules, and one draw needn't show every extreme that they name: `tile_source`: index into the partition's source table; every source block from 16 onward is named by at least one live slot of the partition. `counts`: slots at or past a row block's count are padding, whatever their tiles hold; a partition's live slots together number at least 48. `requests`: block numbers within the asked partition; repeats may occur. `send_ids`: block numbers within the sending partition; repeats may occur.
All inputs are finite; a program needn't handle non-finite values.
Results may differ from the reference program's by a relative error of at most 0.007.
Values may be sent and summed in bfloat16 or wider, within the bound.
No kernel may reach another device: no remote copies, remote signals or barrier semaphores. Data moves between devices by JAX's collectives and lax.ppermute only.
A program may use at most 64 MiB of HBM per device.

```python
import jax
import jax.numpy as jnp
from jax import lax

FEAT = 128
BLK = 128
NB = 16
KMAX = 8
REQ = 1
NBND = 2
NODES = 524288
NSRC = 64
N_GRP = 8
N_MEM = 32


def live_counts(key):
    remote = NSRC - NB
    lowest = min(KMAX, (remote + NB - 1) // NB)
    light_top = min(KMAX, lowest + 1)
    heavy_low = max(lowest, KMAX - KMAX // 4)
    level_key, fill_key = jax.random.split(jax.random.fold_in(key, 7))
    level = jax.random.randint(level_key, (N_GRP, N_MEM, 1), 0, 2)
    level = level.at[0, 0, 0].set(1).at[N_GRP - 1, N_MEM - 1, 0].set(0)
    bottom = jnp.where(level == 1, heavy_low, lowest)
    top = jnp.where(level == 1, KMAX, light_top)
    drawn = jax.random.randint(fill_key, (N_GRP, N_MEM, NB), 0, 1048576)
    result = bottom + drawn % (top - bottom + 1)
    result = result.at[0, 0, 0].set(KMAX).at[N_GRP - 1, N_MEM - 1, 0].set(lowest)
    return result.astype(jnp.int32)


def draw_counts(key, part):
    return live_counts(key)


def draw_tile_source(key, part):
    live_per_row = live_counts(key)
    remote = NSRC - NB
    slots_all = NB * KMAX
    parts_all = N_GRP * N_MEM
    order_key, fill_key = jax.random.split(jax.random.fold_in(key, 11))
    order_bits = jax.random.randint(order_key, (parts_all, slots_all), 0, 1048576)
    filler = jax.random.randint(fill_key, (parts_all, slots_all), 0, NSRC)
    live = (jnp.arange(KMAX, dtype=jnp.int32)[None, None, None, :] < live_per_row[..., None]).reshape(parts_all, slots_all)
    score = order_bits * slots_all + jnp.arange(slots_all, dtype=jnp.int32)[None, :] + jnp.where(live, 0, 268435456)
    ranks = jnp.argsort(jnp.argsort(score, axis=1, stable=True), axis=1, stable=True).astype(jnp.int32)
    source = jnp.where(ranks < remote, NB + ranks, jnp.where(ranks < remote + NB, ranks - remote, filler))
    return source.reshape(N_GRP, N_MEM, NB, KMAX).astype(jnp.int32)


def place_ends(values, rng, least, largest):
    place = [jax.random.randint(jax.random.fold_in(rng, axis), (), 0, length) for axis, length in enumerate(values.shape)]
    main_axis = values.shape.index(max(values.shape))
    beside = place[:main_axis] + [(place[main_axis] + 1) % values.shape[main_axis]] + place[main_axis + 1:]
    return values.at[tuple(place)].set(least).at[tuple(beside)].set(largest)


def block_levels(stream_key, dims, shards, least, high):
    def one(axis_at, shards_of):
        steps = jax.random.uniform(jax.random.fold_in(jax.random.fold_in(stream_key, 6), axis_at), (shards_of,), jnp.float32, least / len(shards), high / len(shards))
        return jnp.repeat(jnp.exp(steps), dims[axis_at] // shards_of).reshape((-1,) + (1,) * (len(dims) - axis_at - 1))

    loudness = one(*shards[0])
    for cut in shards[1:]:
        loudness = loudness * one(*cut)
    return loudness


def bell_draw(rng, dims, scale, reach, cuts=(), kind=jnp.bfloat16):
    entries = jax.random.normal(rng, dims, jnp.float32) * scale
    if len(cuts) > 0:
        entries = block_levels(rng, dims, cuts, -0.22, 0.18) * entries
    return jnp.clip(entries, min=-reach, max=reach).astype(kind)


def setup_inputs(seed: int = 0) -> dict:
    key_of = jax.random.split(jax.random.key(seed), 11)
    return {
        "layer_input": bell_draw(key_of[0], (NODES, FEAT), 1.0, 6.0, ((0, 256),)),
        "history": bell_draw(key_of[1], (NODES, FEAT), 1.0, 6.0, ((0, 256),)),
        "adjacency": jnp.clip(0.049804688 * jax.random.uniform(key_of[2], (N_GRP, N_MEM, NB, KMAX, BLK, BLK), jnp.float32) ** block_levels(key_of[2], (N_GRP, N_MEM, NB, KMAX, BLK, BLK), ((0, 8), (1, 32)), -0.2, 0.2), 0.0, 0.049804688).astype(jnp.bfloat16),
        "tile_source": draw_tile_source(jax.random.fold_in(key_of[10], 71), 0),
        "counts": draw_counts(jax.random.fold_in(key_of[10], 71), 0),
        "requests": place_ends(jax.random.randint(key_of[5], (N_GRP, N_MEM, N_MEM, REQ), 0, NB), jax.random.fold_in(key_of[5], 1), 0, NB - 1).astype(jnp.int32),
        "send_ids": place_ends(jax.random.randint(key_of[6], (N_GRP, N_MEM, N_GRP, NBND), 0, NB), jax.random.fold_in(key_of[6], 1), 0, NB - 1).astype(jnp.int32),
        "weight": bell_draw(key_of[7], (FEAT, FEAT), FEAT ** -0.5, 0.5),
        "layer_bias": bell_draw(key_of[8], (FEAT,), 0.5, 3.0, (), jnp.float32),
        "cotangent": bell_draw(key_of[9], (NODES, FEAT), 1.0, 6.0, ((0, 256),)),
    }


def activate(values):
    return jax.nn.gelu(values, approximate=True)

def reference(layer_input, history, adjacency, tile_source, counts, requests, send_ids, weight, layer_bias, cotangent):
    history_all = history.reshape(N_GRP, N_MEM, NB, BLK, FEAT)
    current_all = layer_input.reshape(N_GRP, N_MEM, NB, BLK, FEAT)
    cotangent_all = cotangent.reshape(N_GRP, N_MEM, NB * BLK, FEAT)
    member_ids = jnp.arange(N_MEM, dtype=jnp.int32)[:, None]
    group_ids = jnp.arange(N_GRP, dtype=jnp.int32)[:, None]
    block_ids = jnp.arange(NB, dtype=jnp.int32)
    slot_ids = jnp.arange(KMAX, dtype=jnp.int32)

    def device_step(device):
        group_pos = device // N_MEM
        member_pos = device % N_MEM
        fetched = history_all[group_pos][member_ids, requests[group_pos, member_pos]]
        border = history_all[group_ids, member_pos, send_ids[:, member_pos, group_pos]]
        source_table = jnp.concatenate([current_all[group_pos, member_pos], fetched.reshape(-1, BLK, FEAT), border.reshape(-1, BLK, FEAT)], axis=0)
        source_ids = tile_source[group_pos, member_pos]
        sources = source_table[source_ids]
        live_slots = slot_ids[None, :] < counts[group_pos, member_pos][:, None]
        masked = jnp.where(live_slots[:, :, None, None], adjacency[group_pos, member_pos], jnp.zeros((), adjacency.dtype))
        aggregate = jnp.einsum('rkij,rkjc->ric', masked.astype(jnp.float32), sources.astype(jnp.float32))
        aggregate = aggregate.reshape(NB * BLK, FEAT).astype(jnp.bfloat16)
        pre_act = jnp.dot(aggregate, weight, preferred_element_type=jnp.float32) + layer_bias
        output = activate(pre_act).astype(jnp.bfloat16)
        grad_pre = jax.vjp(activate, pre_act)[1](cotangent_all[group_pos, member_pos].astype(pre_act.dtype))[0].astype(jnp.bfloat16)
        weight_term = jnp.einsum('nf,ng->fg', aggregate.astype(jnp.float32), grad_pre.astype(jnp.float32))
        bias_term = lax.optimization_barrier(jnp.sum(grad_pre.astype(jnp.float32), axis=0))
        grad_agg = jnp.dot(grad_pre, weight.T, preferred_element_type=jnp.float32).astype(jnp.bfloat16).reshape(NB, BLK, FEAT)
        spread = jnp.einsum('rkij,ric->rkjc', masked.astype(jnp.float32), grad_agg.astype(jnp.float32))
        onehot = ((source_ids[:, :, None] == block_ids[None, None, :]) & live_slots[:, :, None]).astype(jnp.float32)
        grad_local = jnp.dot(onehot.reshape(NB * KMAX, NB).T, spread.reshape(NB * KMAX, BLK * FEAT), precision=lax.Precision.HIGHEST)
        grad_local = grad_local.reshape(NB * BLK, FEAT).astype(jnp.bfloat16)
        return (output, grad_local, weight_term, bias_term)
    outputs, input_grads, weight_terms, bias_terms = lax.map(device_step, jnp.arange(N_GRP * N_MEM, dtype=jnp.int32))
    loss_scale = NODES ** (-0.5)
    layer_output = outputs.reshape(NODES, FEAT)
    input_grad = input_grads.reshape(NODES, FEAT)
    weight_grad = lax.optimization_barrier(jnp.sum(weight_terms, axis=0)) * loss_scale
    bias_grad = lax.optimization_barrier(jnp.sum(bias_terms, axis=0)) * loss_scale
    return (layer_output, input_grad, weight_grad, bias_grad)
```

```python
import jax
import jax.numpy as jnp
from jax import lax
from jax.experimental import pallas as pl
from jax.experimental.pallas import tpu as pltpu
from jax.sharding import Mesh
from jax.sharding import PartitionSpec as P

MEM = ("mem_0", "mem_1")
GRP = ("grp_0", "grp_1")
GRP_MEM = ("grp_0", "grp_1", "mem_0", "mem_1")
F32 = jnp.float32
BF16 = jnp.bfloat16
CHUNKS = 4
ROOT = 0.7978845608028654
CUBIC = 0.044715


def shifted(values, axis, by):
    size = lax.axis_size(axis)
    return lax.ppermute(values, axis, [(i, (i + by) % size) for i in range(size)])


def summed_by_four(values, axis):
    one, two, three = (shifted(values, axis, by) for by in (1, 2, 3))
    return (values + two) + (one + three)


def forward_kernel(
    place, counts, core, adjacency, local, fetched, border_a, border_b, weight, bias, cotangent,
    output, grad_pre, kept, sent,
    tiles, table, aggregate, sems,
):
    rows, slots, block, features = tiles.shape
    copies = [
        pltpu.make_async_copy(adjacency.at[r], tiles.at[r], sems.at[r]) for r in range(rows)
    ]
    for copy in copies:
        copy.start()
    first = 0
    for part in (local, fetched, border_a, border_b):
        table[pl.ds(first, part.shape[0])] = part[...]
        first += part.shape[0]
    for r in range(rows):
        copies[r].wait()
        left, right = [], []
        for k in range(slots):
            tile = tiles[r, k]
            left.append(jnp.where(k < counts[r], tile, jnp.zeros_like(tile)))
            right.append(table[place[r * slots + k]])
        total = jnp.dot(
            jnp.concatenate(left, axis=1),
            jnp.concatenate(right, axis=0),
            preferred_element_type=F32,
        )
        aggregate[pl.ds(r * block, block), :] = total.astype(BF16)
    lines = rows * block // CHUNKS
    weight_term = jnp.zeros((features, features), F32)
    bias_term = jnp.zeros((1, features), F32)
    for i in range(CHUNKS):
        at = pl.ds(i * lines, lines)
        agg = aggregate[at, :]
        v = jnp.dot(agg, weight[...], preferred_element_type=F32) + bias[...]
        square = v * v
        t = jnp.tanh(ROOT * (v * (1.0 + CUBIC * square)))
        half = 0.5 * (1.0 + t)
        output[at, :] = (v * half).astype(BF16)
        slope = half + (0.5 * ROOT) * v * (1.0 - t * t) * (1.0 + (3.0 * CUBIC) * square)
        grad = (cotangent[at, :].astype(F32) * slope).astype(BF16)
        grad_pre[at, :] = grad
        weight_term += lax.dot_general(
            agg, grad, (((0,), (0,)), ((), ())), preferred_element_type=F32
        )
        bias_term += jnp.sum(grad.astype(F32), axis=0, keepdims=True)
    half_rows = features // 2
    upper, lower = weight_term[:half_rows], weight_term[half_rows:]
    is_first = core[0] == 0
    kept[pl.ds(0, half_rows), :] = jnp.where(is_first, upper, lower)
    sent[pl.ds(0, half_rows), :] = jnp.where(is_first, lower, upper)
    tail = jnp.broadcast_to(bias_term, (8, features))
    kept[pl.ds(half_rows, 8), :] = tail
    sent[pl.ds(half_rows, 8), :] = tail


def backward_kernel(
    place, adjacency, grad_pre, weight, input_grad, tiles, sums, sems
):
    rows, slots, block, features = tiles.shape
    copies = [
        pltpu.make_async_copy(adjacency.at[r], tiles.at[r], sems.at[r]) for r in range(rows)
    ]
    for copy in copies:
        copy.start()
    sums[...] = jnp.zeros(sums.shape, F32)
    for r in range(rows):
        grad_agg = lax.dot_general(
            weight[...],
            grad_pre[pl.ds(r * block, block), :],
            (((1,), (1,)), ((), ())),
            preferred_element_type=F32,
        ).astype(BF16)
        copies[r].wait()
        for k in range(slots):
            at = place[r * slots + k]
            sums[at] += jnp.dot(grad_agg, tiles[r, k], preferred_element_type=F32)
    for c in range(rows):
        input_grad[pl.ds(c * block, block), :] = sums[c].T.astype(BF16)


def per_device(
    layer_input, history, adjacency, tile_source, counts, requests, send_ids, weight, layer_bias,
    cotangent,
):
    rows, slots, block = adjacency.shape[2:5]
    features = layer_input.shape[1]
    far, near = GRP
    far_size, near_size = lax.axis_size(far), lax.axis_size(near)
    members = lax.axis_size(MEM)
    groups = far_size * near_size
    at_far, at_near = lax.axis_index(far), lax.axis_index(near)
    blocks = history.reshape(rows, block, features)

    wanted = lax.all_to_all(requests[0, 0], MEM, split_axis=0, concat_axis=0, tiled=True)

    each = send_ids.shape[-1]
    ids = send_ids[0, 0].reshape(far_size, near_size, each)
    far_order = (at_far + jnp.arange(far_size, dtype=jnp.int32)) % far_size
    near_order = (at_near + jnp.arange(near_size, dtype=jnp.int32)) % near_size
    order = (far_order[:, None] * near_size + near_order[None, :]).reshape(-1)
    ids = ids.reshape(groups, each).at[order].get(mode="promise_in_bounds")
    outgoing = blocks.at[ids.reshape(-1)].get(mode="promise_in_bounds")
    outgoing = outgoing.reshape(far_size, near_size * each, block, features)
    arrived = [outgoing[0]] + [shifted(outgoing[by], far, by) for by in range(1, far_size)]
    border_a = jnp.concatenate([a[:each] for a in arrived], axis=0)
    border_b = shifted(jnp.concatenate([a[each:] for a in arrived], axis=0), near, 1)

    served = blocks.at[wanted.reshape(-1)].get(mode="promise_in_bounds")
    fetched = lax.all_to_all(served, MEM, split_axis=0, concat_axis=0, tiled=True)

    source = tile_source[0, 0].reshape(-1)
    first_border = rows + members
    group = (source - first_border) // each
    side = (group % near_size != at_near).astype(jnp.int32)
    hop = (at_far - group // near_size) % far_size
    moved = first_border + side * (far_size * each) + hop * each + (source - first_border) % each
    place = jnp.where(source < first_border, source, moved)
    live_counts = counts[0, 0]
    live = (
        jnp.arange(slots, dtype=jnp.int32)[None, :] < live_counts[:, None]
    ).reshape(-1)
    target = jnp.where(live & (source < rows), source, rows)

    nodes = rows * block
    vmem = pl.BlockSpec(memory_space=pltpu.VMEM)
    smem = pl.BlockSpec(memory_space=pltpu.SMEM)
    anywhere = pl.BlockSpec(memory_space=pl.ANY)
    half_rows = features // 2 + 8
    tiles = pltpu.VMEM((rows, slots, block, features), BF16)
    layer_output, grad_pre, kept, sent = pl.pallas_call(
        forward_kernel,
        out_shape=(
            jax.ShapeDtypeStruct((nodes, features), BF16),
            jax.ShapeDtypeStruct((nodes, features), BF16),
            jax.ShapeDtypeStruct((half_rows, features), F32),
            jax.ShapeDtypeStruct((half_rows, features), F32),
        ),
        in_specs=[smem, smem, smem, anywhere, vmem, vmem, vmem, vmem, vmem, vmem, vmem],
        out_specs=(vmem, vmem, vmem, vmem),
        scratch_shapes=[
            tiles,
            pltpu.VMEM((rows + members + groups * each, block, features), BF16),
            pltpu.VMEM((nodes, features), BF16),
            pltpu.SemaphoreType.DMA((rows,)),
        ],
        name="forward",
    )(
        place, live_counts, at_near.reshape(1), adjacency[0, 0],
        layer_input.reshape(rows, block, features), fetched, border_a, border_b,
        weight, layer_bias.reshape(1, features), cotangent,
    )
    total = kept + shifted(sent, near, 1)
    total = summed_by_four(total, far)
    total = summed_by_four(total, MEM[0])
    depth = lax.axis_size(MEM[1])
    total = lax.all_to_all(
        jnp.broadcast_to(total[None], (depth, *total.shape)), MEM[1], 0, 0, tiled=True
    ).sum(axis=0)
    other = shifted(total, near, 1)
    input_grad = pl.pallas_call(
        backward_kernel,
        out_shape=jax.ShapeDtypeStruct((nodes, features), BF16),
        in_specs=[smem, anywhere, vmem, vmem],
        out_specs=vmem,
        scratch_shapes=[
            tiles,
            pltpu.VMEM((rows + 1, block, features), F32),
            pltpu.SemaphoreType.DMA((rows,)),
        ],
        cost_estimate=pl.CostEstimate(
            flops=2 * rows * slots * block * block * features,
            bytes_accessed=2 * rows * slots * block * block,
            transcendentals=0,
        ),
        name="backward",
    )(target, adjacency[0, 0], grad_pre, weight)
    scale = (nodes * groups * members) ** (-0.5)
    total, other = total * scale, other * scale
    mine, theirs = total[: features // 2], other[: features // 2]
    is_first = at_near == 0
    weight_grad = jnp.concatenate(
        [jnp.where(is_first, mine, theirs), jnp.where(is_first, theirs, mine)], axis=0
    )
    return layer_output, input_grad, weight_grad, total[features // 2]


def solution(mesh):
    finer = Mesh(mesh.devices.reshape(4, 2, 4, 8), ("grp_0", "grp_1", "mem_0", "mem_1"))
    placed = (
        P(GRP_MEM, None),
        P(GRP_MEM, None),
        P(GRP, MEM, None, None, None, None),
        P(GRP, MEM, None, None),
        P(GRP, MEM, None),
        P(GRP, MEM, None, None),
        P(GRP, MEM, None, None),
        P(),
        P(),
        P(GRP_MEM, None),
    )
    return jax.shard_map(
        per_device,
        mesh=finer,
        in_specs=placed,
        out_specs=(P(GRP_MEM, None), P(GRP_MEM, None), P(), P()),
        check_vma=False,
    )
```

```python
import functools

import jax
import jax.numpy as jnp
from jax import lax
from jax.experimental import pallas as pl
from jax.experimental.pallas import tpu as pltpu
from jax.sharding import Mesh
from jax.sharding import PartitionSpec as P

MEM = ("mem_0", "mem_1")
GRP = ("grp_0", "grp_1")
GRP_MEM = ("grp_0", "grp_1", "mem_0", "mem_1")
F32 = jnp.float32
BF16 = jnp.bfloat16
CHUNKS = 4
ROOT = 0.7978845608028654
CUBIC = 0.044715
SPARE = 8
AHEAD = 3
GROUP = 4


def shifted(values, axis, by):
    size = lax.axis_size(axis)
    return lax.ppermute(values, axis, [(i, (i + by) % size) for i in range(size)])


def all_four(values, axis):
    return (values, *(shifted(values, axis, by) for by in (1, 2, 3)))


def forward_kernel(
    place, adjacency, local, fetched, border_a, border_b, weight, bias, cotangent,
    output, grad_pre, term,
    tiles, table, aggregate, cotangents, out_rows, grad_rows, load_sems, side_sem, store_sems,
):
    rows, slots, block, features = tiles.shape
    sources = table.shape[0]
    loads = []
    for r in range(0, rows, GROUP):
        part = pl.ds(r, GROUP)
        loads.append(
            pltpu.make_async_copy(adjacency.at[part], tiles.at[part], load_sems.at[r // GROUP])
        )
    for load in loads[:AHEAD]:
        load.start()
    side = pltpu.make_async_copy(cotangent, cotangents, side_sem)
    side.start()
    first = 0
    for part in (local, fetched, border_a, border_b):
        table[pl.ds(first, part.shape[0])] = part[...]
        first += part.shape[0]
    for r in range(rows):
        if r % GROUP == 0:
            loads[r // GROUP].wait()
            if r // GROUP + AHEAD < len(loads):
                loads[r // GROUP + AHEAD].start()
        left, right = [], []
        for k in range(slots):
            at = place[r * slots + k]
            tile = tiles[r, k]
            left.append(jnp.where(at < sources, tile, jnp.zeros_like(tile)))
            right.append(table[at % sources])
        total = jnp.dot(
            jnp.concatenate(left, axis=1),
            jnp.concatenate(right, axis=0),
            preferred_element_type=F32,
        )
        aggregate[pl.ds(r * block, block), :] = total.astype(BF16)
    side.wait()
    lines = rows * block // CHUNKS
    weight_term = jnp.zeros((features, features), F32)
    bias_term = jnp.zeros((1, features), F32)
    stores = []
    for i in range(CHUNKS):
        at = pl.ds(i * lines, lines)
        agg = aggregate[at, :]
        v = jnp.dot(agg, weight[...], preferred_element_type=F32) + bias[...]
        square = v * v
        t = jnp.tanh(ROOT * (v * (1.0 + CUBIC * square)))
        half = 0.5 * (1.0 + t)
        out_rows[at, :] = (v * half).astype(BF16)
        slope = half + (0.5 * ROOT) * v * (1.0 - t * t) * (1.0 + (3.0 * CUBIC) * square)
        grad = (cotangents[at, :].astype(F32) * slope).astype(BF16)
        grad_rows[at, :] = grad
        for j, (here, there) in enumerate(((out_rows, output), (grad_rows, grad_pre))):
            store = pltpu.make_async_copy(here.at[at, :], there.at[at, :], store_sems.at[i, j])
            store.start()
            stores.append(store)
        weight_term += lax.dot_general(
            agg, grad, (((0,), (0,)), ((), ())), preferred_element_type=F32
        )
        bias_term += jnp.sum(grad.astype(F32), axis=0, keepdims=True)
    term[pl.ds(0, features), :] = weight_term
    term[pl.ds(features, SPARE), :] = jnp.broadcast_to(bias_term, (SPARE, features))
    for store in stores:
        store.wait()


def backward_kernel(target, adjacency, grad_pre, weight, input_grad, tiles, sums, load_sems):
    rows, slots, block, _ = tiles.shape
    loads = []
    for r in range(0, rows, GROUP):
        part = pl.ds(r, GROUP)
        loads.append(
            pltpu.make_async_copy(adjacency.at[part], tiles.at[part], load_sems.at[r // GROUP])
        )
    for load in loads[:AHEAD]:
        load.start()
    sums[...] = jnp.zeros(sums.shape, F32)
    grad_agg = lax.dot_general(
        weight[...], grad_pre[...], (((1,), (1,)), ((), ())), preferred_element_type=F32
    ).astype(BF16)
    for r in range(rows):
        if r % GROUP == 0:
            loads[r // GROUP].wait()
            if r // GROUP + AHEAD < len(loads):
                loads[r // GROUP + AHEAD].start()
        spread = jnp.dot(
            grad_agg[:, r * block : (r + 1) * block],
            jnp.concatenate([tiles[r, k] for k in range(slots)], axis=1),
            preferred_element_type=F32,
        )
        for k in range(slots):
            sums[target[r * slots + k]] += spread[:, k * block : (k + 1) * block]
    for c in range(rows):
        input_grad[pl.ds(c * block, block), :] = sums[c].T.astype(BF16)


def pair_kernel(a, b, out):
    out[...] = a[...] + b[...]


def four_kernel(a, b, c, d, out):
    out[...] = (a[...] + c[...]) + (b[...] + d[...])


def copies_kernel(a, b, c, d, out):
    total = (a[...] + c[...]) + (b[...] + d[...])
    tail = total[total.shape[0] - SPARE :]
    rest = tail - tail.astype(BF16).astype(F32)
    packed = jnp.concatenate([total, rest], axis=0).astype(BF16)
    for i in range(out.shape[0]):
        out[i] = packed


def last_kernel(scale, copies, weight_grad, bias_grad):
    total = copies[0].astype(F32)
    for i in range(1, copies.shape[0]):
        total += copies[i].astype(F32)
    features = weight_grad.shape[0]
    weight_grad[...] = total[:features] * scale
    both = total[features : features + SPARE] + total[features + SPARE :]
    bias_grad[...] = both[:1] * scale


VMEM = pl.BlockSpec(memory_space=pltpu.VMEM)
SMEM = pl.BlockSpec(memory_space=pltpu.SMEM)
ANY = pl.BlockSpec(memory_space=pltpu.HBM)


def local_call(kernel, outs, *args, specs=None, out_specs=None, scratch=(), flops=0, limit=2):
    return pl.pallas_call(
        kernel,
        out_shape=[jax.ShapeDtypeStruct(*out) for out in outs],
        in_specs=specs or [VMEM] * len(args),
        out_specs=out_specs or [VMEM] * len(outs),
        scratch_shapes=list(scratch),
        compiler_params=pltpu.CompilerParams(vmem_limit_bytes=limit * 2**20),
        cost_estimate=pl.CostEstimate(flops=flops, bytes_accessed=0, transcendentals=0)
        if flops
        else None,
    )(*args)


def per_device(
    layer_input, history, adjacency, tile_source, counts, requests, send_ids, weight, layer_bias,
    cotangent,
):
    rows, slots, block = adjacency.shape[2:5]
    features = layer_input.shape[1]
    far, near = GRP
    far_size, near_size = lax.axis_size(far), lax.axis_size(near)
    members = lax.axis_size(MEM)
    groups = far_size * near_size
    at_far, at_near = lax.axis_index(far), lax.axis_index(near)
    blocks = history.reshape(rows, block, features)

    asked = requests[0, 0].reshape(1, 1, -1)
    asked = lax.all_to_all(
        jnp.broadcast_to(asked, (members, 1, asked.shape[2])), MEM, 0, 0, tiled=True
    )
    at_member = lax.axis_index(MEM)
    mine = jnp.arange(asked.shape[2], dtype=jnp.int32) == at_member
    wanted = jnp.sum(jnp.where(mine[None, None, :], asked, 0), axis=(1, 2))

    each = send_ids.shape[-1]
    ids = send_ids[0, 0].reshape(far_size, near_size, each)
    far_order = (at_far + jnp.arange(far_size, dtype=jnp.int32)) % far_size
    near_order = (at_near + jnp.arange(near_size, dtype=jnp.int32)) % near_size
    order = (far_order[:, None] * near_size + near_order[None, :]).reshape(-1)
    ids = ids.reshape(groups, each).at[order].get(mode="promise_in_bounds")
    outgoing = blocks.at[ids.reshape(-1)].get(mode="promise_in_bounds")
    outgoing = outgoing.reshape(far_size, near_size * each, block, features)
    arrived = [outgoing[0]] + [shifted(outgoing[by], far, by) for by in range(1, far_size)]
    border_a = jnp.concatenate([a[:each] for a in arrived], axis=0)
    border_b = shifted(jnp.concatenate([a[each:] for a in arrived], axis=0), near, 1)

    served = blocks.at[wanted.reshape(-1)].get(mode="promise_in_bounds")
    fetched = lax.all_to_all(served, MEM, split_axis=0, concat_axis=0, tiled=True)

    source = tile_source[0, 0].reshape(-1)
    first_border = rows + members
    group = (source - first_border) // each
    side = (group % near_size != at_near).astype(jnp.int32)
    hop = (at_far - group // near_size) % far_size
    moved = first_border + side * (far_size * each) + hop * each + (source - first_border) % each
    place = jnp.where(source < first_border, source, moved)
    live = (
        jnp.arange(slots, dtype=jnp.int32)[None, :] < counts[0, 0][:, None]
    ).reshape(-1)
    sources = rows + members + groups * each
    place = jnp.where(live, place, sources)
    target = jnp.where(live & (source < rows), source, rows)

    nodes = rows * block
    tiles = pltpu.with_memory_space_constraint(adjacency[0, 0], pltpu.HBM)
    whole, terms = ((nodes, features), BF16), ((features + SPARE, features), F32)
    loaded = pltpu.VMEM(tiles.shape, BF16)
    load_sems = pltpu.SemaphoreType.DMA((rows,))
    layer_output, grad_pre, term = local_call(
        forward_kernel,
        [whole, whole, terms],
        place, tiles, layer_input.reshape(rows, block, features), fetched, border_a, border_b,
        weight, layer_bias.reshape(1, features),
        pltpu.with_memory_space_constraint(cotangent, pltpu.HBM),
        specs=[SMEM, ANY] + [VMEM] * 6 + [ANY],
        out_specs=[ANY, ANY, VMEM],
        scratch=[
            loaded,
            pltpu.VMEM((sources, block, features), BF16),
            *(pltpu.VMEM((nodes, features), BF16) for _ in range(4)),
            load_sems,
            pltpu.SemaphoreType.DMA(()),
            pltpu.SemaphoreType.DMA((CHUNKS, 2)),
        ],
        limit=24,
    )
    part = (term.shape, F32)
    (total,) = local_call(pair_kernel, [part], term, shifted(term, near, 1))
    (total,) = local_call(four_kernel, [part], *all_four(total, far))
    depth = lax.axis_size(MEM[1])
    (copies,) = local_call(
        copies_kernel,
        [((depth, features + 2 * SPARE, features), BF16)],
        *all_four(total, MEM[0]),
    )
    copies = lax.all_to_all(copies, MEM[1], 0, 0, tiled=True)
    (input_grad,) = local_call(
        backward_kernel,
        [whole],
        target, tiles, grad_pre, weight,
        specs=[SMEM, ANY, VMEM, VMEM],
        scratch=[loaded, pltpu.VMEM((rows + 1, block, features), F32), load_sems],
        flops=2 * rows * slots * block * block * features,
        limit=24,
    )
    scale = (nodes * groups * members) ** (-0.5)
    weight_grad, bias_grad = local_call(
        functools.partial(last_kernel, scale),
        [((features, features), F32), ((1, features), F32)],
        copies,
    )
    return layer_output, input_grad, weight_grad, bias_grad.reshape(features)


def solution(mesh):
    finer = Mesh(mesh.devices.reshape(4, 2, 4, 8), ("grp_0", "grp_1", "mem_0", "mem_1"))
    placed = (
        P(GRP_MEM, None),
        P(GRP_MEM, None),
        P(GRP, MEM, None, None, None, None),
        P(GRP, MEM, None, None),
        P(GRP, MEM, None),
        P(GRP, MEM, None, None),
        P(GRP, MEM, None, None),
        P(),
        P(),
        P(GRP_MEM, None),
    )
    return jax.shard_map(
        per_device,
        mesh=finer,
        in_specs=placed,
        out_specs=(P(GRP_MEM, None), P(GRP_MEM, None), P(), P()),
        check_vma=False,
    )
```

```python
import functools

import jax
import jax.numpy as jnp
from jax import lax
from jax.experimental import pallas as pl
from jax.experimental.pallas import tpu as pltpu
from jax.sharding import Mesh
from jax.sharding import PartitionSpec as P

MEM = ("mem_0", "mem_1")
GRP = ("grp_0", "grp_1")
GRP_MEM = ("grp_0", "grp_1", "mem_0", "mem_1")
F32 = jnp.float32
BF16 = jnp.bfloat16
CHUNKS = 4
ROOT = 0.7978845608028654
CUBIC = 0.044715
SPARE = 8
GROUP = 4
HEAD = 3


def shifted(values, axis, by):
    size = lax.axis_size(axis)
    return lax.ppermute(values, axis, [(i, (i + by) % size) for i in range(size)])


def all_four(values, axis):
    return (values, *(shifted(values, axis, by) for by in (1, 2, 3)))


def started(source, target, sems, firsts):
    loads = {}
    for i, r in enumerate(firsts):
        part = pl.ds(r, min(GROUP, source.shape[0] - r))
        loads[r] = pltpu.make_async_copy(source.at[part], target.at[part], sems.at[i])
        loads[r].start()
    return loads


def forward_kernel(
    place_in, adjacency, head, local, fetched, border_a, border_b, weight, bias, cotangent,
    output, grad_pre, term,
    place, tiles, table, aggregate, cotangents, out_rows, grad_rows, load_sems, side_sems,
    store_sems,
):
    index = pltpu.make_async_copy(place_in, place, side_sems.at[0])
    index.start()
    rows, slots, block, features = tiles.shape
    sources = table.shape[0]
    ready = head.shape[0]
    loads = started(adjacency, tiles, load_sems, range(ready, rows, GROUP))
    side = pltpu.make_async_copy(cotangent, cotangents, side_sems.at[1])
    side.start()
    first = 0
    for part in (local, fetched, border_a, border_b):
        table[pl.ds(first, part.shape[0])] = part[...]
        first += part.shape[0]
    index.wait()
    for r in range(rows):
        if r in loads:
            loads[r].wait()
        left, right = [], []
        for k in range(slots):
            at = place[r * slots + k]
            tile = head[r, k] if r < ready else tiles[r, k]
            left.append(jnp.where(at < sources, tile, jnp.zeros_like(tile)))
            right.append(table[at % sources])
        total = jnp.dot(
            jnp.concatenate(left, axis=1),
            jnp.concatenate(right, axis=0),
            preferred_element_type=F32,
        )
        aggregate[pl.ds(r * block, block), :] = total.astype(BF16)
    side.wait()
    lines = rows * block // CHUNKS
    weight_term = jnp.zeros((features, features), F32)
    bias_term = jnp.zeros((1, features), F32)
    stores = []
    for i in range(CHUNKS):
        at = pl.ds(i * lines, lines)
        agg = aggregate[at, :]
        v = jnp.dot(agg, weight[...], preferred_element_type=F32) + bias[...]
        square = v * v
        t = jnp.tanh(ROOT * (v * (1.0 + CUBIC * square)))
        half = 0.5 * (1.0 + t)
        out_rows[at, :] = (v * half).astype(BF16)
        slope = half + (0.5 * ROOT) * v * (1.0 - t * t) * (1.0 + (3.0 * CUBIC) * square)
        grad = (cotangents[at, :].astype(F32) * slope).astype(BF16)
        grad_rows[at, :] = grad
        for j, (here, there) in enumerate(((out_rows, output), (grad_rows, grad_pre))):
            store = pltpu.make_async_copy(here.at[at, :], there.at[at, :], store_sems.at[i, j])
            store.start()
            stores.append(store)
        weight_term += lax.dot_general(
            agg, grad, (((0,), (0,)), ((), ())), preferred_element_type=F32
        )
        bias_term += jnp.sum(grad.astype(F32), axis=0, keepdims=True)
    term[pl.ds(0, features), :] = weight_term
    term[pl.ds(features, SPARE), :] = jnp.broadcast_to(bias_term, (SPARE, features))
    for store in stores:
        store.wait()


def backward_kernel(
    target_in, adjacency, grad_pre, weight, input_grad, target, tiles, sums, load_sems, side_sem
):
    index = pltpu.make_async_copy(target_in, target, side_sem)
    index.start()
    rows, slots, block, _ = tiles.shape
    loads = started(adjacency, tiles, load_sems, range(0, rows, GROUP))
    sums[...] = jnp.zeros(sums.shape, F32)
    grad_agg = lax.dot_general(
        weight[...], grad_pre[...], (((1,), (1,)), ((), ())), preferred_element_type=F32
    ).astype(BF16)
    index.wait()
    for r in range(rows):
        if r in loads:
            loads[r].wait()
        spread = jnp.dot(
            grad_agg[:, r * block : (r + 1) * block],
            jnp.concatenate([tiles[r, k] for k in range(slots)], axis=1),
            preferred_element_type=F32,
        )
        for k in range(slots):
            sums[target[r * slots + k]] += spread[:, k * block : (k + 1) * block]
    for c in range(rows):
        input_grad[pl.ds(c * block, block), :] = sums[c].T.astype(BF16)


def pair_kernel(a, b, out):
    out[...] = a[...] + b[...]


def four_kernel(a, b, c, d, out):
    out[...] = (a[...] + c[...]) + (b[...] + d[...])


def copies_kernel(a, b, c, d, out):
    total = (a[...] + c[...]) + (b[...] + d[...])
    tail = total[total.shape[0] - SPARE :]
    rest = tail - tail.astype(BF16).astype(F32)
    packed = jnp.concatenate([total, rest], axis=0).astype(BF16)
    for i in range(out.shape[0]):
        out[i] = packed


def last_kernel(scale, copies, weight_grad, bias_grad):
    total = copies[0].astype(F32)
    for i in range(1, copies.shape[0]):
        total += copies[i].astype(F32)
    features = weight_grad.shape[0]
    weight_grad[...] = total[:features] * scale
    both = total[features : features + SPARE] + total[features + SPARE :]
    bias_grad[...] = both[:1] * scale


VMEM = pl.BlockSpec(memory_space=pltpu.VMEM)
ANY = pl.BlockSpec(memory_space=pltpu.HBM)


def local_call(kernel, outs, *args, specs=None, out_specs=None, scratch=(), flops=0, limit=2):
    return pl.pallas_call(
        kernel,
        out_shape=outs,
        in_specs=specs or [VMEM] * len(args),
        out_specs=out_specs or [VMEM] * len(outs),
        scratch_shapes=list(scratch),
        compiler_params=pltpu.CompilerParams(vmem_limit_bytes=limit * 2**20),
        cost_estimate=pl.CostEstimate(flops=flops, bytes_accessed=0, transcendentals=0)
        if flops
        else None,
    )(*args)


def per_device(
    layer_input, history, adjacency, tile_source, counts, requests, send_ids, weight, layer_bias,
    cotangent,
):
    rows, slots, block = adjacency.shape[2:5]
    features = layer_input.shape[1]
    far, near = GRP
    far_size, near_size = lax.axis_size(far), lax.axis_size(near)
    members = lax.axis_size(MEM)
    groups = far_size * near_size
    at_far, at_near = lax.axis_index(far), lax.axis_index(near)
    blocks = history.reshape(rows, block, features)

    asked = requests[0, 0].reshape(1, 1, -1)
    asked = lax.all_to_all(
        jnp.broadcast_to(asked, (members, 1, asked.shape[2])), MEM, 0, 0, tiled=True
    )
    at_member = lax.axis_index(MEM)
    mine = jnp.arange(asked.shape[2], dtype=jnp.int32) == at_member
    wanted = jnp.sum(jnp.where(mine[None, None, :], asked, 0), axis=(1, 2))

    each = send_ids.shape[-1]
    ids = send_ids[0, 0].reshape(far_size, near_size, each)
    far_order = (at_far + jnp.arange(far_size, dtype=jnp.int32)) % far_size
    near_order = (at_near + jnp.arange(near_size, dtype=jnp.int32)) % near_size
    order = (far_order[:, None] * near_size + near_order[None, :]).reshape(-1)
    ids = ids.reshape(groups, each).at[order].get(mode="promise_in_bounds")
    outgoing = blocks.at[ids.reshape(-1)].get(mode="promise_in_bounds")
    outgoing = outgoing.reshape(far_size, near_size * each, block, features)
    arrived = [outgoing[0]] + [shifted(outgoing[by], far, by) for by in range(1, far_size)]
    border_a = jnp.concatenate([a[:each] for a in arrived], axis=0)
    border_b = shifted(jnp.concatenate([a[each:] for a in arrived], axis=0), near, 1)

    served = blocks.at[wanted.reshape(-1)].get(mode="promise_in_bounds")
    fetched = lax.all_to_all(served, MEM, split_axis=0, concat_axis=0, tiled=True)

    source = tile_source[0, 0].reshape(-1)
    first_border = rows + members
    group = (source - first_border) // each
    side = (group % near_size != at_near).astype(jnp.int32)
    hop = (at_far - group // near_size) % far_size
    moved = first_border + side * (far_size * each) + hop * each + (source - first_border) % each
    place = jnp.where(source < first_border, source, moved)
    live = (
        jnp.arange(slots, dtype=jnp.int32)[None, :] < counts[0, 0][:, None]
    ).reshape(-1)
    sources = rows + members + groups * each
    place = jnp.where(live, place, sources)
    target = jnp.where(live & (source < rows), source, rows)

    nodes = rows * block
    tiles = pltpu.with_memory_space_constraint(adjacency[0, 0], pltpu.HBM)
    whole = jax.ShapeDtypeStruct((nodes, features), BF16)
    stored = pltpu.HBM((nodes, features), BF16)
    term_shape = jax.ShapeDtypeStruct((features + SPARE, features), F32)
    head = pltpu.with_memory_space_constraint(adjacency[0, 0, :HEAD], pltpu.VMEM)
    loaded = pltpu.VMEM(tiles.shape, BF16)
    table_of = pltpu.SMEM((rows * slots,), jnp.int32)
    load_sems = pltpu.SemaphoreType.DMA((rows,))
    layer_output, grad_pre, term = local_call(
        forward_kernel,
        [stored, stored, term_shape],
        place, tiles, head, layer_input.reshape(rows, block, features), fetched, border_a, border_b,
        weight, layer_bias.reshape(1, features),
        pltpu.with_memory_space_constraint(cotangent, pltpu.HBM),
        specs=[ANY, ANY] + [VMEM] * 7 + [ANY],
        out_specs=[ANY, ANY, VMEM],
        scratch=[
            table_of,
            loaded,
            pltpu.VMEM((sources, block, features), BF16),
            *(pltpu.VMEM((nodes, features), BF16) for _ in range(4)),
            load_sems,
            pltpu.SemaphoreType.DMA((2,)),
            pltpu.SemaphoreType.DMA((CHUNKS, 2)),
        ],
        limit=24,
    )
    (total,) = local_call(pair_kernel, [term_shape], term, shifted(term, near, 1))
    (total,) = local_call(four_kernel, [term_shape], *all_four(total, far))
    depth = lax.axis_size(MEM[1])
    (copies,) = local_call(
        copies_kernel,
        [jax.ShapeDtypeStruct((depth, features + 2 * SPARE, features), BF16)],
        *all_four(total, MEM[0]),
    )
    copies = lax.all_to_all(copies, MEM[1], 0, 0, tiled=True)
    (input_grad,) = local_call(
        backward_kernel,
        [whole],
        target, tiles, grad_pre, weight,
        specs=[ANY, ANY, VMEM, VMEM],
        scratch=[
            table_of,
            loaded,
            pltpu.VMEM((rows + 1, block, features), F32),
            load_sems,
            pltpu.SemaphoreType.DMA(()),
        ],
        flops=2 * rows * slots * block * block * features,
        limit=24,
    )
    scale = (nodes * groups * members) ** (-0.5)
    weight_grad, bias_grad = local_call(
        functools.partial(last_kernel, scale),
        [
            jax.ShapeDtypeStruct((features, features), F32),
            jax.ShapeDtypeStruct((1, features), F32),
        ],
        copies,
    )
    return layer_output, input_grad, weight_grad, bias_grad.reshape(features)


def solution(mesh):
    finer = Mesh(mesh.devices.reshape(4, 2, 4, 8), ("grp_0", "grp_1", "mem_0", "mem_1"))
    placed = (
        P(GRP_MEM, None),
        P(GRP_MEM, None),
        P(GRP, MEM, None, None, None, None),
        P(GRP, MEM, None, None),
        P(GRP, MEM, None),
        P(GRP, MEM, None, None),
        P(GRP, MEM, None, None),
        P(),
        P(),
        P(GRP_MEM, None),
    )
    return jax.shard_map(
        per_device,
        mesh=finer,
        in_specs=placed,
        out_specs=(P(GRP_MEM, None), P(GRP_MEM, None), P(), P()),
        check_vma=False,
    )
```

```python
import functools

import jax
import jax.numpy as jnp
from jax import lax
from jax.experimental import pallas as pl
from jax.experimental.pallas import tpu as pltpu
from jax.sharding import Mesh
from jax.sharding import PartitionSpec as P

MEM = ("mem_0", "mem_1")
GRP = ("grp_0", "grp_1")
GRP_MEM = ("grp_0", "grp_1", "mem_0", "mem_1")
F32 = jnp.float32
BF16 = jnp.bfloat16
CHUNKS = 4
ROOT = 0.7978845608028654
CUBIC = 0.044715
SPARE = 8
GROUP = 4
HEAD = 3


def shifted(values, axis, by):
    size = lax.axis_size(axis)
    return lax.ppermute(values, axis, [(i, (i + by) % size) for i in range(size)])


def all_four(values, axis):
    return (values, *(shifted(values, axis, by) for by in (1, 2, 3)))


def started(source, target, sems, firsts):
    loads = {}
    for i, r in enumerate(firsts):
        part = pl.ds(r, min(GROUP, source.shape[0] - r))
        loads[r] = pltpu.make_async_copy(source.at[part], target.at[part], sems.at[i])
        loads[r].start()
    return loads


def forward_kernel(
    place_in, adjacency, head, local, fetched, border_a, border_b, weight, bias, cotangent,
    output, grad_pre, term,
    place, tiles, table, aggregate, cotangents, out_rows, grad_rows, load_sems, side_sems,
    store_sems,
):
    index = pltpu.make_async_copy(place_in, place, side_sems.at[0])
    index.start()
    rows, slots, block, features = tiles.shape
    sources = table.shape[0]
    ready = head.shape[0]
    loads = started(adjacency, tiles, load_sems, range(ready, rows, GROUP))
    side = pltpu.make_async_copy(cotangent, cotangents, side_sems.at[1])
    side.start()
    first = 0
    for part in (local, fetched, border_a, border_b):
        table[pl.ds(first, part.shape[0])] = part[...]
        first += part.shape[0]
    index.wait()
    for r in range(rows):
        if r in loads:
            loads[r].wait()
        left, right = [], []
        for k in range(slots):
            at = place[r * slots + k]
            tile = head[r, k] if r < ready else tiles[r, k]
            left.append(jnp.where(at < sources, tile, jnp.zeros_like(tile)))
            right.append(table[at % sources])
        total = jnp.dot(
            jnp.concatenate(left, axis=1),
            jnp.concatenate(right, axis=0),
            preferred_element_type=F32,
        )
        aggregate[pl.ds(r * block, block), :] = total.astype(BF16)
    side.wait()
    lines = rows * block // CHUNKS
    weight_term = jnp.zeros((features, features), F32)
    bias_term = jnp.zeros((1, features), F32)
    stores = []
    for i in range(CHUNKS):
        at = pl.ds(i * lines, lines)
        agg = aggregate[at, :]
        v = jnp.dot(agg, weight[...], preferred_element_type=F32) + bias[...]
        square = v * v
        t = jnp.tanh(ROOT * (v * (1.0 + CUBIC * square)))
        half = 0.5 * (1.0 + t)
        out_rows[at, :] = (v * half).astype(BF16)
        slope = half + (0.5 * ROOT) * v * (1.0 - t * t) * (1.0 + (3.0 * CUBIC) * square)
        grad = (cotangents[at, :].astype(F32) * slope).astype(BF16)
        grad_rows[at, :] = grad
        for j, (here, there) in enumerate(((out_rows, output), (grad_rows, grad_pre))):
            store = pltpu.make_async_copy(here.at[at, :], there.at[at, :], store_sems.at[i, j])
            store.start()
            stores.append(store)
        weight_term += lax.dot_general(
            agg, grad, (((0,), (0,)), ((), ())), preferred_element_type=F32
        )
        bias_term += jnp.sum(grad.astype(F32), axis=0, keepdims=True)
    term[pl.ds(0, features), :] = weight_term
    term[pl.ds(features, SPARE), :] = jnp.broadcast_to(bias_term, (SPARE, features))
    for store in stores:
        store.wait()


def backward_kernel(
    target_in, adjacency, grad_pre, weight, input_grad, target, tiles, sums, load_sems, side_sem
):
    index = pltpu.make_async_copy(target_in, target, side_sem)
    index.start()
    rows, slots, block, _ = tiles.shape
    loads = started(adjacency, tiles, load_sems, range(0, rows, GROUP))
    sums[...] = jnp.zeros(sums.shape, F32)
    grad_agg = lax.dot_general(
        weight[...], grad_pre[...], (((1,), (1,)), ((), ())), preferred_element_type=F32
    ).astype(BF16)
    index.wait()
    for r in range(rows):
        if r in loads:
            loads[r].wait()
        spread = jnp.dot(
            grad_agg[:, r * block : (r + 1) * block],
            jnp.concatenate([tiles[r, k] for k in range(slots)], axis=1),
            preferred_element_type=F32,
        )
        for k in range(slots):
            sums[target[r * slots + k]] += spread[:, k * block : (k + 1) * block]
    for c in range(rows):
        input_grad[pl.ds(c * block, block), :] = sums[c].T.astype(BF16)


def pair_kernel(a, b, core, out):
    total = a[...] + b[...]
    half = (total.shape[0] - SPARE) // 2
    first = core[:1] == 0
    out[:half] = jnp.where(first, total[:half], total[half : 2 * half])
    out[half:] = total[2 * half :]


def four_kernel(a, b, c, d, out):
    out[...] = (a[...] + c[...]) + (b[...] + d[...])


def copies_kernel(a, b, c, d, out):
    total = (a[...] + c[...]) + (b[...] + d[...])
    tail = total[total.shape[0] - SPARE :]
    rest = tail - tail.astype(BF16).astype(F32)
    packed = jnp.concatenate([total, rest], axis=0).astype(BF16)
    for i in range(out.shape[0]):
        out[i] = packed


def last_kernel(scale, cores, copies, weight_grad, bias_grad):
    half = weight_grad.shape[0] // cores
    each = copies.shape[0] // cores
    for core in range(cores):
        total = copies[core * each].astype(F32)
        for i in range(1, each):
            total += copies[core * each + i].astype(F32)
        weight_grad[pl.ds(core * half, half)] = total[:half] * scale
        if core == 0:
            both = total[half : half + SPARE] + total[half + SPARE :]
            bias_grad[...] = both[:1] * scale


VMEM = pl.BlockSpec(memory_space=pltpu.VMEM)
ANY = pl.BlockSpec(memory_space=pltpu.HBM)


def local_call(kernel, outs, *args, specs=None, out_specs=None, scratch=(), flops=0, limit=2):
    return pl.pallas_call(
        kernel,
        out_shape=outs,
        in_specs=specs or [VMEM] * len(args),
        out_specs=out_specs or [VMEM] * len(outs),
        scratch_shapes=list(scratch),
        compiler_params=pltpu.CompilerParams(vmem_limit_bytes=limit * 2**20),
        cost_estimate=pl.CostEstimate(flops=flops, bytes_accessed=0, transcendentals=0)
        if flops
        else None,
    )(*args)


def per_device(
    layer_input, history, adjacency, tile_source, counts, requests, send_ids, weight, layer_bias,
    cotangent,
):
    rows, slots, block = adjacency.shape[2:5]
    features = layer_input.shape[1]
    far, near = GRP
    far_size, near_size = lax.axis_size(far), lax.axis_size(near)
    members = lax.axis_size(MEM)
    groups = far_size * near_size
    at_far, at_near = lax.axis_index(far), lax.axis_index(near)
    blocks = history.reshape(rows, block, features)

    asked = requests[0, 0].reshape(1, 1, -1)
    asked = lax.all_to_all(
        jnp.broadcast_to(asked, (members, 1, asked.shape[2])), MEM, 0, 0, tiled=True
    )
    at_member = lax.axis_index(MEM)
    mine = jnp.arange(asked.shape[2], dtype=jnp.int32) == at_member
    wanted = jnp.sum(jnp.where(mine[None, None, :], asked, 0), axis=(1, 2))

    each = send_ids.shape[-1]
    ids = send_ids[0, 0].reshape(far_size, near_size, each)
    far_order = (at_far + jnp.arange(far_size, dtype=jnp.int32)) % far_size
    near_order = (at_near + jnp.arange(near_size, dtype=jnp.int32)) % near_size
    order = (far_order[:, None] * near_size + near_order[None, :]).reshape(-1)
    ids = ids.reshape(groups, each).at[order].get(mode="promise_in_bounds")
    outgoing = blocks.at[ids.reshape(-1)].get(mode="promise_in_bounds")
    outgoing = outgoing.reshape(far_size, near_size * each, block, features)
    arrived = [outgoing[0]] + [shifted(outgoing[by], far, by) for by in range(1, far_size)]
    border_a = jnp.concatenate([a[:each] for a in arrived], axis=0)
    border_b = shifted(jnp.concatenate([a[each:] for a in arrived], axis=0), near, 1)

    served = blocks.at[wanted.reshape(-1)].get(mode="promise_in_bounds")
    fetched = lax.all_to_all(served, MEM, split_axis=0, concat_axis=0, tiled=True)

    source = tile_source[0, 0].reshape(-1)
    first_border = rows + members
    group = (source - first_border) // each
    side = (group % near_size != at_near).astype(jnp.int32)
    hop = (at_far - group // near_size) % far_size
    moved = first_border + side * (far_size * each) + hop * each + (source - first_border) % each
    place = jnp.where(source < first_border, source, moved)
    live = (
        jnp.arange(slots, dtype=jnp.int32)[None, :] < counts[0, 0][:, None]
    ).reshape(-1)
    sources = rows + members + groups * each
    place = jnp.where(live, place, sources)
    target = jnp.where(live & (source < rows), source, rows)

    nodes = rows * block
    tiles = pltpu.with_memory_space_constraint(adjacency[0, 0], pltpu.HBM)
    whole = jax.ShapeDtypeStruct((nodes, features), BF16)
    stored = pltpu.HBM((nodes, features), BF16)
    term_shape = jax.ShapeDtypeStruct((features + SPARE, features), F32)
    head = pltpu.with_memory_space_constraint(adjacency[0, 0, :HEAD], pltpu.VMEM)
    loaded = pltpu.VMEM(tiles.shape, BF16)
    table_of = pltpu.SMEM((rows * slots,), jnp.int32)
    load_sems = pltpu.SemaphoreType.DMA((rows,))
    layer_output, grad_pre, term = local_call(
        forward_kernel,
        [stored, stored, term_shape],
        place, tiles, head, layer_input.reshape(rows, block, features), fetched, border_a, border_b,
        weight, layer_bias.reshape(1, features),
        pltpu.with_memory_space_constraint(cotangent, pltpu.HBM),
        specs=[ANY, ANY] + [VMEM] * 7 + [ANY],
        out_specs=[ANY, ANY, VMEM],
        scratch=[
            table_of,
            loaded,
            pltpu.VMEM((sources, block, features), BF16),
            *(pltpu.VMEM((nodes, features), BF16) for _ in range(4)),
            load_sems,
            pltpu.SemaphoreType.DMA((2,)),
            pltpu.SemaphoreType.DMA((CHUNKS, 2)),
        ],
        limit=24,
    )
    half_shape = jax.ShapeDtypeStruct((features // near_size + SPARE, features), F32)
    core = jnp.full((SPARE, features), at_near, jnp.int32)
    (total,) = local_call(pair_kernel, [half_shape], term, shifted(term, near, 1), core)
    (total,) = local_call(four_kernel, [half_shape], *all_four(total, far))
    last_axes = (near, MEM[1])
    peers = lax.axis_size(last_axes)
    packed = (peers, half_shape.shape[0] + SPARE, features)
    (copies,) = local_call(
        copies_kernel, [jax.ShapeDtypeStruct(packed, BF16)], *all_four(total, MEM[0])
    )
    copies = lax.all_to_all(copies, last_axes, 0, 0, tiled=True)
    (input_grad,) = local_call(
        backward_kernel,
        [whole],
        target, tiles, grad_pre, weight,
        specs=[ANY, ANY, VMEM, VMEM],
        scratch=[
            table_of,
            loaded,
            pltpu.VMEM((rows + 1, block, features), F32),
            load_sems,
            pltpu.SemaphoreType.DMA(()),
        ],
        flops=2 * rows * slots * block * block * features,
        limit=24,
    )
    scale = (nodes * groups * members) ** (-0.5)
    weight_grad, bias_grad = local_call(
        functools.partial(last_kernel, scale, near_size),
        [
            jax.ShapeDtypeStruct((features, features), F32),
            jax.ShapeDtypeStruct((1, features), F32),
        ],
        copies,
    )
    return layer_output, input_grad, weight_grad, bias_grad.reshape(features)


def solution(mesh):
    finer = Mesh(mesh.devices.reshape(4, 2, 4, 8), ("grp_0", "grp_1", "mem_0", "mem_1"))
    placed = (
        P(GRP_MEM, None),
        P(GRP_MEM, None),
        P(GRP, MEM, None, None, None, None),
        P(GRP, MEM, None, None),
        P(GRP, MEM, None),
        P(GRP, MEM, None, None),
        P(GRP, MEM, None, None),
        P(),
        P(),
        P(GRP_MEM, None),
    )
    return jax.shard_map(
        per_device,
        mesh=finer,
        in_specs=placed,
        out_specs=(P(GRP_MEM, None), P(GRP_MEM, None), P(), P()),
        check_vma=False,
    )
```

```python
import functools

import jax
import jax.numpy as jnp
from jax import lax
from jax.experimental import pallas as pl
from jax.experimental.pallas import tpu as pltpu
from jax.sharding import Mesh
from jax.sharding import PartitionSpec as P

MEM = "mem"
GRP = ("grp_0", "grp_1")
GRP_MEM = ("grp_0", "grp_1", "mem")
NEAR_Y, NEAR_Z = 4, 8
TURN_Y, TURN_Z = 2, 4
TURN_LAST = 4
F32 = jnp.float32
BF16 = jnp.bfloat16
CHUNKS = 4
ROOT = 0.7978845608028654
CUBIC = 0.044715
SPARE = 8
GROUP = 4
HEAD = 3


def shifted(values, axis, by):
    size = lax.axis_size(axis)
    return lax.ppermute(values, axis, [(i, (i + by) % size) for i in range(size)])


def all_four(values, axis):
    return (values, *(shifted(values, axis, by) for by in (1, 2, 3)))


def shifted_rows(values, by):
    size = lax.axis_size(MEM)
    return lax.ppermute(values, MEM, [(i, (i + by * NEAR_Z) % size) for i in range(size)])


def member_order():
    return [
        (y + TURN_Y) % NEAR_Y * NEAR_Z + (z + TURN_Z) % NEAR_Z
        for y in range(NEAR_Y)
        for z in range(NEAR_Z)
    ]


def exchanged(values, groups):
    return lax.all_to_all(values, MEM, 0, 0, axis_index_groups=groups, tiled=True)


def started(source, target, sems, firsts):
    loads = {}
    for i, r in enumerate(firsts):
        part = pl.ds(r, min(GROUP, source.shape[0] - r))
        loads[r] = pltpu.make_async_copy(source.at[part], target.at[part], sems.at[i])
        loads[r].start()
    return loads


def forward_kernel(
    place_in, adjacency, head, local, fetched, border_a, border_b, weight, bias, cotangent,
    output, grad_pre, term,
    place, tiles, table, aggregate, cotangents, out_rows, grad_rows, load_sems, side_sems,
    store_sems,
):
    index = pltpu.make_async_copy(place_in, place, side_sems.at[0])
    index.start()
    rows, slots, block, features = tiles.shape
    sources = table.shape[0]
    ready = head.shape[0]
    loads = started(adjacency, tiles, load_sems, range(ready, rows, GROUP))
    side = pltpu.make_async_copy(cotangent, cotangents, side_sems.at[1])
    side.start()
    first = 0
    for part in (local, fetched, border_a, border_b):
        table[pl.ds(first, part.shape[0])] = part[...]
        first += part.shape[0]
    index.wait()
    for r in range(rows):
        if r in loads:
            loads[r].wait()
        left, right = [], []
        for k in range(slots):
            at = place[r * slots + k]
            tile = head[r, k] if r < ready else tiles[r, k]
            left.append(jnp.where(at < sources, tile, jnp.zeros_like(tile)))
            right.append(table[at % sources])
        total = jnp.dot(
            jnp.concatenate(left, axis=1),
            jnp.concatenate(right, axis=0),
            preferred_element_type=F32,
        )
        aggregate[pl.ds(r * block, block), :] = total.astype(BF16)
    side.wait()
    lines = rows * block // CHUNKS
    weight_term = jnp.zeros((features, features), F32)
    bias_term = jnp.zeros((1, features), F32)
    stores = []
    for i in range(CHUNKS):
        at = pl.ds(i * lines, lines)
        agg = aggregate[at, :]
        v = jnp.dot(agg, weight[...], preferred_element_type=F32) + bias[...]
        square = v * v
        t = jnp.tanh(ROOT * (v * (1.0 + CUBIC * square)))
        half = 0.5 * (1.0 + t)
        out_rows[at, :] = (v * half).astype(BF16)
        slope = half + (0.5 * ROOT) * v * (1.0 - t * t) * (1.0 + (3.0 * CUBIC) * square)
        grad = (cotangents[at, :].astype(F32) * slope).astype(BF16)
        grad_rows[at, :] = grad
        for j, (here, there) in enumerate(((out_rows, output), (grad_rows, grad_pre))):
            store = pltpu.make_async_copy(here.at[at, :], there.at[at, :], store_sems.at[i, j])
            store.start()
            stores.append(store)
        weight_term += lax.dot_general(
            agg, grad, (((0,), (0,)), ((), ())), preferred_element_type=F32
        )
        bias_term += jnp.sum(grad.astype(F32), axis=0, keepdims=True)
    term[pl.ds(0, features), :] = weight_term
    term[pl.ds(features, SPARE), :] = jnp.broadcast_to(bias_term, (SPARE, features))
    for store in stores:
        store.wait()


def backward_kernel(
    target_in, adjacency, grad_pre, weight, input_grad, target, tiles, sums, load_sems, side_sem
):
    index = pltpu.make_async_copy(target_in, target, side_sem)
    index.start()
    rows, slots, block, _ = tiles.shape
    loads = started(adjacency, tiles, load_sems, range(0, rows, GROUP))
    sums[...] = jnp.zeros(sums.shape, F32)
    grad_agg = lax.dot_general(
        weight[...], grad_pre[...], (((1,), (1,)), ((), ())), preferred_element_type=F32
    ).astype(BF16)
    index.wait()
    for r in range(rows):
        if r in loads:
            loads[r].wait()
        spread = jnp.dot(
            grad_agg[:, r * block : (r + 1) * block],
            jnp.concatenate([tiles[r, k] for k in range(slots)], axis=1),
            preferred_element_type=F32,
        )
        for k in range(slots):
            sums[target[r * slots + k]] += spread[:, k * block : (k + 1) * block]
    for c in range(rows):
        input_grad[pl.ds(c * block, block), :] = sums[c].T.astype(BF16)


def pair_kernel(a, b, out):
    out[...] = a[...] + b[...]


def four_kernel(a, b, c, d, out):
    out[...] = (a[...] + c[...]) + (b[...] + d[...])


def copies_kernel(a, b, c, d, out):
    total = (a[...] + c[...]) + (b[...] + d[...])
    tail = total[total.shape[0] - SPARE :]
    rest = tail - tail.astype(BF16).astype(F32)
    packed = jnp.concatenate([total, rest], axis=0).astype(BF16)
    for i in range(out.shape[0]):
        out[i] = packed


def last_kernel(scale, copies, weight_grad, bias_grad):
    total = copies[0].astype(F32)
    for i in range(1, copies.shape[0]):
        total += copies[i].astype(F32)
    features = weight_grad.shape[0]
    weight_grad[...] = total[:features] * scale
    both = total[features : features + SPARE] + total[features + SPARE :]
    bias_grad[...] = both[:1] * scale


VMEM = pl.BlockSpec(memory_space=pltpu.VMEM)
ANY = pl.BlockSpec(memory_space=pltpu.HBM)


def local_call(kernel, outs, *args, specs=None, out_specs=None, scratch=(), flops=0, limit=2):
    return pl.pallas_call(
        kernel,
        out_shape=outs,
        in_specs=specs or [VMEM] * len(args),
        out_specs=out_specs or [VMEM] * len(outs),
        scratch_shapes=list(scratch),
        compiler_params=pltpu.CompilerParams(vmem_limit_bytes=limit * 2**20),
        cost_estimate=pl.CostEstimate(flops=flops, bytes_accessed=0, transcendentals=0)
        if flops
        else None,
    )(*args)


def per_device(
    layer_input, history, adjacency, tile_source, counts, requests, send_ids, weight, layer_bias,
    cotangent,
):
    rows, slots, block = adjacency.shape[2:5]
    features = layer_input.shape[1]
    far, near = GRP
    far_size, near_size = lax.axis_size(far), lax.axis_size(near)
    members = lax.axis_size(MEM)
    groups = far_size * near_size
    at_far, at_near = lax.axis_index(far), lax.axis_index(near)
    blocks = history.reshape(rows, block, features)

    asked = requests[0, 0].reshape(1, 1, -1)
    asked = exchanged(jnp.broadcast_to(asked, (members, 1, asked.shape[2])), [member_order()])
    at_member = lax.axis_index(MEM)
    mine = jnp.arange(asked.shape[2], dtype=jnp.int32) == at_member
    wanted = jnp.sum(jnp.where(mine[None, None, :], asked, 0), axis=(1, 2))

    each = send_ids.shape[-1]
    ids = send_ids[0, 0].reshape(far_size, near_size, each)
    far_order = (at_far + jnp.arange(far_size, dtype=jnp.int32)) % far_size
    near_order = (at_near + jnp.arange(near_size, dtype=jnp.int32)) % near_size
    order = (far_order[:, None] * near_size + near_order[None, :]).reshape(-1)
    ids = ids.reshape(groups, each).at[order].get(mode="promise_in_bounds")
    outgoing = blocks.at[ids.reshape(-1)].get(mode="promise_in_bounds")
    outgoing = outgoing.reshape(far_size, near_size * each, block, features)
    arrived = [outgoing[0]] + [shifted(outgoing[by], far, by) for by in range(1, far_size)]
    border_a = jnp.concatenate([a[:each] for a in arrived], axis=0)
    border_b = shifted(jnp.concatenate([a[each:] for a in arrived], axis=0), near, 1)

    served = blocks.at[wanted.reshape(-1)].get(mode="promise_in_bounds")
    fetched = exchanged(served, [member_order()])

    source = tile_source[0, 0].reshape(-1)
    first_border = rows + members
    group = (source - first_border) // each
    side = (group % near_size != at_near).astype(jnp.int32)
    hop = (at_far - group // near_size) % far_size
    moved = first_border + side * (far_size * each) + hop * each + (source - first_border) % each
    member = source - rows
    turned = (member // NEAR_Z - TURN_Y) % NEAR_Y * NEAR_Z + (member - TURN_Z) % NEAR_Z
    inner = jnp.where(source < rows, source, rows + turned)
    place = jnp.where(source < first_border, inner, moved)
    live = (
        jnp.arange(slots, dtype=jnp.int32)[None, :] < counts[0, 0][:, None]
    ).reshape(-1)
    sources = rows + members + groups * each
    place = jnp.where(live, place, sources)
    target = jnp.where(live & (source < rows), source, rows)

    nodes = rows * block
    tiles = pltpu.with_memory_space_constraint(adjacency[0, 0], pltpu.HBM)
    whole = jax.ShapeDtypeStruct((nodes, features), BF16)
    stored = pltpu.HBM((nodes, features), BF16)
    term_shape = jax.ShapeDtypeStruct((features + SPARE, features), F32)
    head = pltpu.with_memory_space_constraint(adjacency[0, 0, :HEAD], pltpu.VMEM)
    loaded = pltpu.VMEM(tiles.shape, BF16)
    table_of = pltpu.SMEM((rows * slots,), jnp.int32)
    load_sems = pltpu.SemaphoreType.DMA((rows,))
    layer_output, grad_pre, term = local_call(
        forward_kernel,
        [stored, stored, term_shape],
        place, tiles, head, layer_input.reshape(rows, block, features), fetched, border_a, border_b,
        weight, layer_bias.reshape(1, features),
        pltpu.with_memory_space_constraint(cotangent, pltpu.HBM),
        specs=[ANY, ANY] + [VMEM] * 7 + [ANY],
        out_specs=[ANY, ANY, VMEM],
        scratch=[
            table_of,
            loaded,
            pltpu.VMEM((sources, block, features), BF16),
            *(pltpu.VMEM((nodes, features), BF16) for _ in range(4)),
            load_sems,
            pltpu.SemaphoreType.DMA((2,)),
            pltpu.SemaphoreType.DMA((CHUNKS, 2)),
        ],
        limit=24,
    )
    (total,) = local_call(pair_kernel, [term_shape], term, shifted(term, near, 1))
    (total,) = local_call(four_kernel, [term_shape], *all_four(total, far))
    depth = NEAR_Z
    (copies,) = local_call(
        copies_kernel,
        [jax.ShapeDtypeStruct((depth, features + 2 * SPARE, features), BF16)],
        total,
        *(shifted_rows(total, by) for by in (1, 2, 3)),
    )
    lines = [
        [y * NEAR_Z + (z + TURN_LAST) % NEAR_Z for z in range(NEAR_Z)] for y in range(NEAR_Y)
    ]
    copies = exchanged(copies, lines)
    (input_grad,) = local_call(
        backward_kernel,
        [whole],
        target, tiles, grad_pre, weight,
        specs=[ANY, ANY, VMEM, VMEM],
        scratch=[
            table_of,
            loaded,
            pltpu.VMEM((rows + 1, block, features), F32),
            load_sems,
            pltpu.SemaphoreType.DMA(()),
        ],
        flops=2 * rows * slots * block * block * features,
        limit=24,
    )
    scale = (nodes * groups * members) ** (-0.5)
    weight_grad, bias_grad = local_call(
        functools.partial(last_kernel, scale),
        [
            jax.ShapeDtypeStruct((features, features), F32),
            jax.ShapeDtypeStruct((1, features), F32),
        ],
        copies,
    )
    return layer_output, input_grad, weight_grad, bias_grad.reshape(features)


def solution(mesh):
    finer = Mesh(mesh.devices.reshape(4, 2, NEAR_Y * NEAR_Z), GRP_MEM)
    placed = (
        P(GRP_MEM, None),
        P(GRP_MEM, None),
        P(GRP, MEM, None, None, None, None),
        P(GRP, MEM, None, None),
        P(GRP, MEM, None),
        P(GRP, MEM, None, None),
        P(GRP, MEM, None, None),
        P(),
        P(),
        P(GRP_MEM, None),
    )
    return jax.shard_map(
        per_device,
        mesh=finer,
        in_specs=placed,
        out_specs=(P(GRP_MEM, None), P(GRP_MEM, None), P(), P()),
        check_vma=False,
    )
```

```python
import functools

import jax
import jax.numpy as jnp
from jax import lax
from jax.experimental import pallas as pl
from jax.experimental.pallas import tpu as pltpu
from jax.sharding import Mesh
from jax.sharding import PartitionSpec as P

MEM = "mem"
GRP = ("grp_0", "grp_1")
GRP_MEM = ("grp_0", "grp_1", "mem")
NEAR_Y, NEAR_Z = 4, 8
TURN_Y, TURN_Z = 2, 4
TURN_LAST = 4
F32 = jnp.float32
BF16 = jnp.bfloat16
CHUNKS = 4
ROOT = 0.7978845608028654
CUBIC = 0.044715
SPARE = 8
GROUP = 4
HEAD = 3


def shifted(values, axis, by):
    size = lax.axis_size(axis)
    return lax.ppermute(values, axis, [(i, (i + by) % size) for i in range(size)])


def partner(values, axis, size, step, flip):
    def other(i):
        at = i // step % size
        return i + ((at ^ flip) - at) * step

    return lax.ppermute(values, axis, [(i, other(i)) for i in range(lax.axis_size(axis))])


def all_four(values, axis, step=1):
    return (values, *(partner(values, axis, 4, step, flip) for flip in (1, 2, 3)))


def member_order():
    return [
        (y + TURN_Y) % NEAR_Y * NEAR_Z + (z + TURN_Z) % NEAR_Z
        for y in range(NEAR_Y)
        for z in range(NEAR_Z)
    ]


def exchanged(values, groups):
    return lax.all_to_all(values, MEM, 0, 0, axis_index_groups=groups, tiled=True)


def started(source, target, sems, firsts):
    loads = {}
    for i, r in enumerate(firsts):
        part = pl.ds(r, min(GROUP, source.shape[0] - r))
        loads[r] = pltpu.make_async_copy(source.at[part], target.at[part], sems.at[i])
        loads[r].start()
    return loads


def forward_kernel(
    place_in, adjacency, head, local, fetched, border_a, border_b, weight, bias, cotangent,
    output, grad_pre, term,
    place, tiles, table, aggregate, cotangents, out_rows, grad_rows, load_sems, side_sems,
    store_sems,
):
    index = pltpu.make_async_copy(place_in, place, side_sems.at[0])
    index.start()
    rows, slots, block, features = tiles.shape
    sources = table.shape[0]
    ready = head.shape[0]
    loads = started(adjacency, tiles, load_sems, range(ready, rows, GROUP))
    side = pltpu.make_async_copy(cotangent, cotangents, side_sems.at[1])
    side.start()
    first = 0
    for part in (local, fetched, border_a, border_b):
        table[pl.ds(first, part.shape[0])] = part[...]
        first += part.shape[0]
    index.wait()
    for r in range(rows):
        if r in loads:
            loads[r].wait()
        left, right = [], []
        for k in range(slots):
            at = place[r * slots + k]
            tile = head[r, k] if r < ready else tiles[r, k]
            left.append(jnp.where(at < sources, tile, jnp.zeros_like(tile)))
            right.append(table[at % sources])
        total = jnp.dot(
            jnp.concatenate(left, axis=1),
            jnp.concatenate(right, axis=0),
            preferred_element_type=F32,
        )
        aggregate[pl.ds(r * block, block), :] = total.astype(BF16)
    side.wait()
    lines = rows * block // CHUNKS
    weight_term = jnp.zeros((features, features), F32)
    bias_term = jnp.zeros((1, features), F32)
    stores = []
    for i in range(CHUNKS):
        at = pl.ds(i * lines, lines)
        agg = aggregate[at, :]
        v = jnp.dot(agg, weight[...], preferred_element_type=F32) + bias[...]
        square = v * v
        t = jnp.tanh(ROOT * (v * (1.0 + CUBIC * square)))
        half = 0.5 * (1.0 + t)
        out_rows[at, :] = (v * half).astype(BF16)
        slope = half + (0.5 * ROOT) * v * (1.0 - t * t) * (1.0 + (3.0 * CUBIC) * square)
        grad = (cotangents[at, :].astype(F32) * slope).astype(BF16)
        grad_rows[at, :] = grad
        for j, (here, there) in enumerate(((out_rows, output), (grad_rows, grad_pre))):
            store = pltpu.make_async_copy(here.at[at, :], there.at[at, :], store_sems.at[i, j])
            store.start()
            stores.append(store)
        weight_term += lax.dot_general(
            agg, grad, (((0,), (0,)), ((), ())), preferred_element_type=F32
        )
        bias_term += jnp.sum(grad.astype(F32), axis=0, keepdims=True)
    term[pl.ds(0, features), :] = weight_term
    term[pl.ds(features, SPARE), :] = jnp.broadcast_to(bias_term, (SPARE, features))
    for store in stores:
        store.wait()


def backward_kernel(
    target_in, adjacency, grad_pre, weight, input_grad, target, tiles, sums, load_sems, side_sem
):
    index = pltpu.make_async_copy(target_in, target, side_sem)
    index.start()
    rows, slots, block, _ = tiles.shape
    loads = started(adjacency, tiles, load_sems, range(0, rows, GROUP))
    sums[...] = jnp.zeros(sums.shape, F32)
    grad_agg = lax.dot_general(
        weight[...], grad_pre[...], (((1,), (1,)), ((), ())), preferred_element_type=F32
    ).astype(BF16)
    index.wait()
    for r in range(rows):
        if r in loads:
            loads[r].wait()
        spread = jnp.dot(
            grad_agg[:, r * block : (r + 1) * block],
            jnp.concatenate([tiles[r, k] for k in range(slots)], axis=1),
            preferred_element_type=F32,
        )
        for k in range(slots):
            sums[target[r * slots + k]] += spread[:, k * block : (k + 1) * block]
    for c in range(rows):
        input_grad[pl.ds(c * block, block), :] = sums[c].T.astype(BF16)


def pair_kernel(a, b, out):
    out[...] = a[...] + b[...]


def four_kernel(a, b, c, d, out):
    out[...] = (a[...] + c[...]) + (b[...] + d[...])


def copies_kernel(a, b, c, d, out):
    total = (a[...] + c[...]) + (b[...] + d[...])
    tail = total[total.shape[0] - SPARE :]
    rest = tail - tail.astype(BF16).astype(F32)
    packed = jnp.concatenate([total, rest], axis=0).astype(BF16)
    for i in range(out.shape[0]):
        out[i] = packed


def last_kernel(scale, copies, weight_grad, bias_grad):
    total = copies[0].astype(F32)
    for i in range(1, copies.shape[0]):
        total += copies[i].astype(F32)
    features = weight_grad.shape[0]
    weight_grad[...] = total[:features] * scale
    both = total[features : features + SPARE] + total[features + SPARE :]
    bias_grad[...] = both[:1] * scale


VMEM = pl.BlockSpec(memory_space=pltpu.VMEM)
ANY = pl.BlockSpec(memory_space=pltpu.HBM)


def local_call(kernel, outs, *args, specs=None, out_specs=None, scratch=(), flops=0, limit=2):
    return pl.pallas_call(
        kernel,
        out_shape=outs,
        in_specs=specs or [VMEM] * len(args),
        out_specs=out_specs or [VMEM] * len(outs),
        scratch_shapes=list(scratch),
        compiler_params=pltpu.CompilerParams(vmem_limit_bytes=limit * 2**20),
        cost_estimate=pl.CostEstimate(flops=flops, bytes_accessed=0, transcendentals=0)
        if flops
        else None,
    )(*args)


def per_device(
    layer_input, history, adjacency, tile_source, counts, requests, send_ids, weight, layer_bias,
    cotangent,
):
    rows, slots, block = adjacency.shape[2:5]
    features = layer_input.shape[1]
    far, near = GRP
    far_size, near_size = lax.axis_size(far), lax.axis_size(near)
    members = lax.axis_size(MEM)
    groups = far_size * near_size
    at_far, at_near = lax.axis_index(far), lax.axis_index(near)
    blocks = history.reshape(rows, block, features)

    asked = requests[0, 0].reshape(1, 1, -1)
    asked = exchanged(jnp.broadcast_to(asked, (members, 1, asked.shape[2])), [member_order()])
    at_member = lax.axis_index(MEM)
    mine = jnp.arange(asked.shape[2], dtype=jnp.int32) == at_member
    wanted = jnp.sum(jnp.where(mine[None, None, :], asked, 0), axis=(1, 2))

    each = send_ids.shape[-1]
    ids = send_ids[0, 0].reshape(far_size, near_size, each)
    far_order = (at_far + jnp.arange(far_size, dtype=jnp.int32)) % far_size
    near_order = (at_near + jnp.arange(near_size, dtype=jnp.int32)) % near_size
    order = (far_order[:, None] * near_size + near_order[None, :]).reshape(-1)
    ids = ids.reshape(groups, each).at[order].get(mode="promise_in_bounds")
    outgoing = blocks.at[ids.reshape(-1)].get(mode="promise_in_bounds")
    outgoing = outgoing.reshape(far_size, near_size * each, block, features)
    arrived = [outgoing[0]] + [shifted(outgoing[by], far, by) for by in range(1, far_size)]
    border_a = jnp.concatenate([a[:each] for a in arrived], axis=0)
    border_b = shifted(jnp.concatenate([a[each:] for a in arrived], axis=0), near, 1)

    served = blocks.at[wanted.reshape(-1)].get(mode="promise_in_bounds")
    fetched = exchanged(served, [member_order()])

    source = tile_source[0, 0].reshape(-1)
    first_border = rows + members
    group = (source - first_border) // each
    side = (group % near_size != at_near).astype(jnp.int32)
    hop = (at_far - group // near_size) % far_size
    moved = first_border + side * (far_size * each) + hop * each + (source - first_border) % each
    member = source - rows
    turned = (member // NEAR_Z - TURN_Y) % NEAR_Y * NEAR_Z + (member - TURN_Z) % NEAR_Z
    inner = jnp.where(source < rows, source, rows + turned)
    place = jnp.where(source < first_border, inner, moved)
    live = (
        jnp.arange(slots, dtype=jnp.int32)[None, :] < counts[0, 0][:, None]
    ).reshape(-1)
    sources = rows + members + groups * each
    place = jnp.where(live, place, sources)
    target = jnp.where(live & (source < rows), source, rows)

    nodes = rows * block
    tiles = pltpu.with_memory_space_constraint(adjacency[0, 0], pltpu.HBM)
    whole = jax.ShapeDtypeStruct((nodes, features), BF16)
    stored = pltpu.HBM((nodes, features), BF16)
    term_shape = jax.ShapeDtypeStruct((features + SPARE, features), F32)
    head = pltpu.with_memory_space_constraint(adjacency[0, 0, :HEAD], pltpu.VMEM)
    loaded = pltpu.VMEM(tiles.shape, BF16)
    table_of = pltpu.SMEM((rows * slots,), jnp.int32)
    load_sems = pltpu.SemaphoreType.DMA((rows,))
    layer_output, grad_pre, term = local_call(
        forward_kernel,
        [stored, stored, term_shape],
        place, tiles, head, layer_input.reshape(rows, block, features), fetched, border_a, border_b,
        weight, layer_bias.reshape(1, features),
        pltpu.with_memory_space_constraint(cotangent, pltpu.HBM),
        specs=[ANY, ANY] + [VMEM] * 7 + [ANY],
        out_specs=[ANY, ANY, VMEM],
        scratch=[
            table_of,
            loaded,
            pltpu.VMEM((sources, block, features), BF16),
            *(pltpu.VMEM((nodes, features), BF16) for _ in range(4)),
            load_sems,
            pltpu.SemaphoreType.DMA((2,)),
            pltpu.SemaphoreType.DMA((CHUNKS, 2)),
        ],
        limit=24,
    )
    (total,) = local_call(pair_kernel, [term_shape], term, shifted(term, near, 1))
    (total,) = local_call(four_kernel, [term_shape], *all_four(total, far))
    depth = NEAR_Z
    (copies,) = local_call(
        copies_kernel,
        [jax.ShapeDtypeStruct((depth, features + 2 * SPARE, features), BF16)],
        *all_four(total, MEM, NEAR_Z),
    )
    lines = [
        [y * NEAR_Z + (z + TURN_LAST) % NEAR_Z for z in range(NEAR_Z)] for y in range(NEAR_Y)
    ]
    copies = exchanged(copies, lines)
    (input_grad,) = local_call(
        backward_kernel,
        [whole],
        target, tiles, grad_pre, weight,
        specs=[ANY, ANY, VMEM, VMEM],
        scratch=[
            table_of,
            loaded,
            pltpu.VMEM((rows + 1, block, features), F32),
            load_sems,
            pltpu.SemaphoreType.DMA(()),
        ],
        flops=2 * rows * slots * block * block * features,
        limit=24,
    )
    scale = (nodes * groups * members) ** (-0.5)
    weight_grad, bias_grad = local_call(
        functools.partial(last_kernel, scale),
        [
            jax.ShapeDtypeStruct((features, features), F32),
            jax.ShapeDtypeStruct((1, features), F32),
        ],
        copies,
    )
    return layer_output, input_grad, weight_grad, bias_grad.reshape(features)


def solution(mesh):
    finer = Mesh(mesh.devices.reshape(4, 2, NEAR_Y * NEAR_Z), GRP_MEM)
    placed = (
        P(GRP_MEM, None),
        P(GRP_MEM, None),
        P(GRP, MEM, None, None, None, None),
        P(GRP, MEM, None, None),
        P(GRP, MEM, None),
        P(GRP, MEM, None, None),
        P(GRP, MEM, None, None),
        P(),
        P(),
        P(GRP_MEM, None),
    )
    return jax.shard_map(
        per_device,
        mesh=finer,
        in_specs=placed,
        out_specs=(P(GRP_MEM, None), P(GRP_MEM, None), P(), P()),
        check_vma=False,
    )
```

```python
import functools

import jax
import jax.numpy as jnp
from jax import lax
from jax.experimental import pallas as pl
from jax.experimental.pallas import tpu as pltpu
from jax.sharding import Mesh
from jax.sharding import PartitionSpec as P

MEM = "mem"
GRP = ("grp_0", "grp_1")
GRP_MEM = ("grp_0", "grp_1", "mem")
NEAR_Y, NEAR_Z = 4, 8
TURN_Y, TURN_Z = 2, 4
TURN_LAST = 4
F32 = jnp.float32
BF16 = jnp.bfloat16
CHUNKS = 4
ROOT = 0.7978845608028654
CUBIC = 0.044715
SPARE = 8
GROUP = 4
HEAD = 3


def shifted(values, axis, by):
    size = lax.axis_size(axis)
    return lax.ppermute(values, axis, [(i, (i + by) % size) for i in range(size)])


def partner(values, axis, size, step, flip):
    def other(i):
        at = i // step % size
        return i + ((at ^ flip) - at) * step

    return lax.ppermute(values, axis, [(i, other(i)) for i in range(lax.axis_size(axis))])


def all_four(values, axis, step=1):
    return (values, *(partner(values, axis, 4, step, flip) for flip in (1, 2, 3)))


def member_order():
    return [
        (y + TURN_Y) % NEAR_Y * NEAR_Z + (z + TURN_Z) % NEAR_Z
        for y in range(NEAR_Y)
        for z in range(NEAR_Z)
    ]


def exchanged(values, groups):
    return lax.all_to_all(values, MEM, 0, 0, axis_index_groups=groups, tiled=True)


def started(source, target, sems, firsts):
    loads = {}
    for i, r in enumerate(firsts):
        part = pl.ds(r, min(GROUP, source.shape[0] - r))
        loads[r] = pltpu.make_async_copy(source.at[part], target.at[part], sems.at[i])
        loads[r].start()
    return loads


def forward_kernel(
    place_in, adjacency, head, local, fetched, border_a, border_b, weight, bias, cotangent,
    output, grad_pre, term,
    place, tiles, table, aggregate, cotangents, out_rows, grad_rows, load_sems, side_sems,
    store_sems,
):
    index = pltpu.make_async_copy(place_in, place, side_sems.at[0])
    index.start()
    rows, slots, block, features = tiles.shape
    sources = table.shape[0]
    ready = head.shape[0]
    loads = started(adjacency, tiles, load_sems, range(ready, rows, GROUP))
    side = pltpu.make_async_copy(cotangent, cotangents, side_sems.at[1])
    side.start()
    first = 0
    for part in (local, fetched, border_a, border_b):
        table[pl.ds(first, part.shape[0])] = part[...]
        first += part.shape[0]
    index.wait()
    for r in range(rows):
        if r in loads:
            loads[r].wait()
        left, right = [], []
        for k in range(slots):
            at = place[r * slots + k]
            tile = head[r, k] if r < ready else tiles[r, k]
            left.append(jnp.where(at < sources, tile, jnp.zeros_like(tile)))
            right.append(table[at % sources])
        total = jnp.dot(
            jnp.concatenate(left, axis=1),
            jnp.concatenate(right, axis=0),
            preferred_element_type=F32,
        )
        aggregate[pl.ds(r * block, block), :] = total.astype(BF16)
    side.wait()
    lines = rows * block // CHUNKS
    weight_term = jnp.zeros((features, features), F32)
    bias_term = jnp.zeros((1, features), F32)
    stores = []
    for i in range(CHUNKS):
        at = pl.ds(i * lines, lines)
        agg = aggregate[at, :]
        v = jnp.dot(agg, weight[...], preferred_element_type=F32) + bias[...]
        square = v * v
        t = jnp.tanh(ROOT * (v * (1.0 + CUBIC * square)))
        half = 0.5 * (1.0 + t)
        out_rows[at, :] = (v * half).astype(BF16)
        slope = half + (0.5 * ROOT) * v * (1.0 - t * t) * (1.0 + (3.0 * CUBIC) * square)
        grad = (cotangents[at, :].astype(F32) * slope).astype(BF16)
        grad_rows[at, :] = grad
        for j, (here, there) in enumerate(((out_rows, output), (grad_rows, grad_pre))):
            store = pltpu.make_async_copy(here.at[at, :], there.at[at, :], store_sems.at[i, j])
            store.start()
            stores.append(store)
        weight_term += lax.dot_general(
            agg, grad, (((0,), (0,)), ((), ())), preferred_element_type=F32
        )
        bias_term += jnp.sum(grad.astype(F32), axis=0, keepdims=True)
    term[pl.ds(0, features), :] = weight_term
    term[pl.ds(features, SPARE), :] = jnp.broadcast_to(bias_term, (SPARE, features))
    for store in stores:
        store.wait()


def backward_kernel(
    target_in, adjacency, grad_pre, weight, input_grad, target, tiles, sums, load_sems, side_sem
):
    index = pltpu.make_async_copy(target_in, target, side_sem)
    index.start()
    rows, slots, block, _ = tiles.shape
    loads = started(adjacency, tiles, load_sems, range(0, rows, GROUP))
    sums[...] = jnp.zeros(sums.shape, F32)
    grad_agg = lax.dot_general(
        weight[...], grad_pre[...], (((1,), (1,)), ((), ())), preferred_element_type=F32
    ).astype(BF16)
    index.wait()
    for r in range(rows):
        if r in loads:
            loads[r].wait()
        spread = jnp.dot(
            grad_agg[:, r * block : (r + 1) * block],
            jnp.concatenate([tiles[r, k] for k in range(slots)], axis=1),
            preferred_element_type=F32,
        )
        for k in range(slots):
            sums[target[r * slots + k]] += spread[:, k * block : (k + 1) * block]
    for c in range(rows):
        input_grad[pl.ds(c * block, block), :] = sums[c].T.astype(BF16)


def packed(total):
    tail = total[total.shape[0] - SPARE :]
    rest = tail - tail.astype(BF16).astype(F32)
    return jnp.concatenate([total, rest], axis=0).astype(BF16)


def unpacked(values):
    wide = values.astype(F32)
    end = wide.shape[0] - SPARE
    return jnp.concatenate([wide[: end - SPARE], wide[end - SPARE : end] + wide[end:]], axis=0)


def pair_kernel(a, b, out):
    out[...] = packed(a[...] + b[...])


def sum_of_four(a, b, c, d):
    return (unpacked(a[...]) + unpacked(c[...])) + (unpacked(b[...]) + unpacked(d[...]))


def four_kernel(a, b, c, d, out):
    out[...] = packed(sum_of_four(a, b, c, d))


def copies_kernel(a, b, c, d, out):
    values = packed(sum_of_four(a, b, c, d))
    for i in range(out.shape[0]):
        out[i] = values


def last_kernel(scale, copies, weight_grad, bias_grad):
    total = copies[0].astype(F32)
    for i in range(1, copies.shape[0]):
        total += copies[i].astype(F32)
    features = weight_grad.shape[0]
    weight_grad[...] = total[:features] * scale
    both = total[features : features + SPARE] + total[features + SPARE :]
    bias_grad[...] = both[:1] * scale


VMEM = pl.BlockSpec(memory_space=pltpu.VMEM)
ANY = pl.BlockSpec(memory_space=pltpu.HBM)


def local_call(kernel, outs, *args, specs=None, out_specs=None, scratch=(), flops=0, limit=2):
    return pl.pallas_call(
        kernel,
        out_shape=outs,
        in_specs=specs or [VMEM] * len(args),
        out_specs=out_specs or [VMEM] * len(outs),
        scratch_shapes=list(scratch),
        compiler_params=pltpu.CompilerParams(vmem_limit_bytes=limit * 2**20),
        cost_estimate=pl.CostEstimate(flops=flops, bytes_accessed=0, transcendentals=0)
        if flops
        else None,
    )(*args)


def per_device(
    layer_input, history, adjacency, tile_source, counts, requests, send_ids, weight, layer_bias,
    cotangent,
):
    rows, slots, block = adjacency.shape[2:5]
    features = layer_input.shape[1]
    far, near = GRP
    far_size, near_size = lax.axis_size(far), lax.axis_size(near)
    members = lax.axis_size(MEM)
    groups = far_size * near_size
    at_far, at_near = lax.axis_index(far), lax.axis_index(near)
    blocks = history.reshape(rows, block, features)

    asked = requests[0, 0].reshape(1, 1, -1)
    asked = exchanged(jnp.broadcast_to(asked, (members, 1, asked.shape[2])), [member_order()])
    at_member = lax.axis_index(MEM)
    mine = jnp.arange(asked.shape[2], dtype=jnp.int32) == at_member
    wanted = jnp.sum(jnp.where(mine[None, None, :], asked, 0), axis=(1, 2))

    each = send_ids.shape[-1]
    ids = send_ids[0, 0].reshape(far_size, near_size, each)
    far_order = (at_far + jnp.arange(far_size, dtype=jnp.int32)) % far_size
    near_order = (at_near + jnp.arange(near_size, dtype=jnp.int32)) % near_size
    order = (far_order[:, None] * near_size + near_order[None, :]).reshape(-1)
    ids = ids.reshape(groups, each).at[order].get(mode="promise_in_bounds")
    outgoing = blocks.at[ids.reshape(-1)].get(mode="promise_in_bounds")
    outgoing = outgoing.reshape(far_size, near_size * each, block, features)
    arrived = [outgoing[0]] + [shifted(outgoing[by], far, by) for by in range(1, far_size)]
    border_a = jnp.concatenate([a[:each] for a in arrived], axis=0)
    border_b = shifted(jnp.concatenate([a[each:] for a in arrived], axis=0), near, 1)

    served = blocks.at[wanted.reshape(-1)].get(mode="promise_in_bounds")
    fetched = exchanged(served, [member_order()])

    source = tile_source[0, 0].reshape(-1)
    first_border = rows + members
    group = (source - first_border) // each
    side = (group % near_size != at_near).astype(jnp.int32)
    hop = (at_far - group // near_size) % far_size
    moved = first_border + side * (far_size * each) + hop * each + (source - first_border) % each
    member = source - rows
    turned = (member // NEAR_Z - TURN_Y) % NEAR_Y * NEAR_Z + (member - TURN_Z) % NEAR_Z
    inner = jnp.where(source < rows, source, rows + turned)
    place = jnp.where(source < first_border, inner, moved)
    live = (
        jnp.arange(slots, dtype=jnp.int32)[None, :] < counts[0, 0][:, None]
    ).reshape(-1)
    sources = rows + members + groups * each
    place = jnp.where(live, place, sources)
    target = jnp.where(live & (source < rows), source, rows)

    nodes = rows * block
    tiles = pltpu.with_memory_space_constraint(adjacency[0, 0], pltpu.HBM)
    whole = jax.ShapeDtypeStruct((nodes, features), BF16)
    stored = pltpu.HBM((nodes, features), BF16)
    term_shape = jax.ShapeDtypeStruct((features + SPARE, features), F32)
    head = pltpu.with_memory_space_constraint(adjacency[0, 0, :HEAD], pltpu.VMEM)
    loaded = pltpu.VMEM(tiles.shape, BF16)
    table_of = pltpu.SMEM((rows * slots,), jnp.int32)
    load_sems = pltpu.SemaphoreType.DMA((rows,))
    layer_output, grad_pre, term = local_call(
        forward_kernel,
        [stored, stored, term_shape],
        place, tiles, head, layer_input.reshape(rows, block, features), fetched, border_a, border_b,
        weight, layer_bias.reshape(1, features),
        pltpu.with_memory_space_constraint(cotangent, pltpu.HBM),
        specs=[ANY, ANY] + [VMEM] * 7 + [ANY],
        out_specs=[ANY, ANY, VMEM],
        scratch=[
            table_of,
            loaded,
            pltpu.VMEM((sources, block, features), BF16),
            *(pltpu.VMEM((nodes, features), BF16) for _ in range(4)),
            load_sems,
            pltpu.SemaphoreType.DMA((2,)),
            pltpu.SemaphoreType.DMA((CHUNKS, 2)),
        ],
        limit=24,
    )
    sent = jax.ShapeDtypeStruct((features + 2 * SPARE, features), BF16)
    (total,) = local_call(pair_kernel, [sent], term, shifted(term, near, 1))
    (total,) = local_call(four_kernel, [sent], *all_four(total, far))
    depth = NEAR_Z
    (copies,) = local_call(
        copies_kernel,
        [jax.ShapeDtypeStruct((depth, features + 2 * SPARE, features), BF16)],
        *all_four(total, MEM, NEAR_Z),
    )
    lines = [
        [y * NEAR_Z + (z + TURN_LAST) % NEAR_Z for z in range(NEAR_Z)] for y in range(NEAR_Y)
    ]
    copies = exchanged(copies, lines)
    (input_grad,) = local_call(
        backward_kernel,
        [whole],
        target, tiles, grad_pre, weight,
        specs=[ANY, ANY, VMEM, VMEM],
        scratch=[
            table_of,
            loaded,
            pltpu.VMEM((rows + 1, block, features), F32),
            load_sems,
            pltpu.SemaphoreType.DMA(()),
        ],
        flops=2 * rows * slots * block * block * features,
        limit=24,
    )
    scale = (nodes * groups * members) ** (-0.5)
    weight_grad, bias_grad = local_call(
        functools.partial(last_kernel, scale),
        [
            jax.ShapeDtypeStruct((features, features), F32),
            jax.ShapeDtypeStruct((1, features), F32),
        ],
        copies,
    )
    return layer_output, input_grad, weight_grad, bias_grad.reshape(features)


def solution(mesh):
    finer = Mesh(mesh.devices.reshape(4, 2, NEAR_Y * NEAR_Z), GRP_MEM)
    placed = (
        P(GRP_MEM, None),
        P(GRP_MEM, None),
        P(GRP, MEM, None, None, None, None),
        P(GRP, MEM, None, None),
        P(GRP, MEM, None),
        P(GRP, MEM, None, None),
        P(GRP, MEM, None, None),
        P(),
        P(),
        P(GRP_MEM, None),
    )
    return jax.shard_map(
        per_device,
        mesh=finer,
        in_specs=placed,
        out_specs=(P(GRP_MEM, None), P(GRP_MEM, None), P(), P()),
        check_vma=False,
    )
```

```python
import functools

import jax
import jax.numpy as jnp
from jax import lax
from jax.experimental import pallas as pl
from jax.experimental.pallas import tpu as pltpu
from jax.sharding import Mesh
from jax.sharding import PartitionSpec as P

MEM = "mem"
GRP = ("grp_0", "grp_1")
GRP_MEM = ("grp_0", "grp_1", "mem")
NEAR_Y, NEAR_Z = 4, 8
TURN_Y, TURN_Z = 2, 4
TURN_LAST = 4
F32 = jnp.float32
BF16 = jnp.bfloat16
CHUNKS = 2
ROOT = 0.7978845608028654
CUBIC = 0.044715
SPARE = 8
GROUP = 7
HEAD = 3


def shifted(values, axis, by):
    size = lax.axis_size(axis)
    return lax.ppermute(values, axis, [(i, (i + by) % size) for i in range(size)])


def partner(values, axis, size, step, flip):
    def other(i):
        at = i // step % size
        return i + ((at ^ flip) - at) * step

    return lax.ppermute(values, axis, [(i, other(i)) for i in range(lax.axis_size(axis))])


def all_four(values, axis, step=1):
    return (values, *(partner(values, axis, 4, step, flip) for flip in (1, 2, 3)))


def member_order():
    return [
        (y + TURN_Y) % NEAR_Y * NEAR_Z + (z + TURN_Z) % NEAR_Z
        for y in range(NEAR_Y)
        for z in range(NEAR_Z)
    ]


def exchanged(values, groups):
    return lax.all_to_all(values, MEM, 0, 0, axis_index_groups=groups, tiled=True)


def started(source, target, sems, firsts):
    loads = {}
    for i, r in enumerate(firsts):
        part = pl.ds(r, min(GROUP, source.shape[0] - r))
        loads[r] = pltpu.make_async_copy(source.at[part], target.at[part], sems.at[i])
        loads[r].start()
    return loads


def forward_kernel(
    place_in, adjacency, head, local, fetched, border_a, border_b, weight, bias, cotangent,
    output, grad_pre, term,
    place, tiles, table, aggregate, cotangents, out_rows, grad_rows, load_sems, side_sems,
    store_sems,
):
    index = pltpu.make_async_copy(place_in, place, side_sems.at[0])
    index.start()
    rows, slots, block, features = tiles.shape
    sources = table.shape[0]
    ready = head.shape[0]
    loads = started(adjacency, tiles, load_sems, range(ready, rows, GROUP))
    side = pltpu.make_async_copy(cotangent, cotangents, side_sems.at[1])
    side.start()
    first = 0
    for part in (local, fetched, border_a, border_b):
        table[pl.ds(first, part.shape[0])] = part[...]
        first += part.shape[0]
    index.wait()
    for r in range(rows):
        if r in loads:
            loads[r].wait()
        left, right = [], []
        for k in range(slots):
            at = place[r * slots + k]
            tile = head[r, k] if r < ready else tiles[r, k]
            left.append(jnp.where(at < sources, tile, jnp.zeros_like(tile)))
            right.append(table[at % sources])
        total = jnp.dot(
            jnp.concatenate(left, axis=1),
            jnp.concatenate(right, axis=0),
            preferred_element_type=F32,
        )
        aggregate[pl.ds(r * block, block), :] = total.astype(BF16)
    side.wait()
    lines = rows * block // CHUNKS
    weight_term = jnp.zeros((features, features), F32)
    bias_term = jnp.zeros((1, features), F32)
    stores = []
    for i in range(CHUNKS):
        at = pl.ds(i * lines, lines)
        agg = aggregate[at, :]
        v = jnp.dot(agg, weight[...], preferred_element_type=F32) + bias[...]
        square = v * v
        t = jnp.tanh(ROOT * (v * (1.0 + CUBIC * square)))
        half = 0.5 * (1.0 + t)
        out_rows[at, :] = (v * half).astype(BF16)
        slope = half + (0.5 * ROOT) * v * (1.0 - t * t) * (1.0 + (3.0 * CUBIC) * square)
        grad = (cotangents[at, :].astype(F32) * slope).astype(BF16)
        grad_rows[at, :] = grad
        for j, (here, there) in enumerate(((out_rows, output), (grad_rows, grad_pre))):
            store = pltpu.make_async_copy(here.at[at, :], there.at[at, :], store_sems.at[i, j])
            store.start()
            stores.append(store)
        weight_term += lax.dot_general(
            agg, grad, (((0,), (0,)), ((), ())), preferred_element_type=F32
        )
        bias_term += jnp.sum(grad.astype(F32), axis=0, keepdims=True)
    term[pl.ds(0, features), :] = weight_term
    term[pl.ds(features, SPARE), :] = jnp.broadcast_to(bias_term, (SPARE, features))
    for store in stores:
        store.wait()


def backward_kernel(
    target_in, adjacency, grad_in, weight, input_grad,
    target, tiles, grad_pre, sums, load_sems, side_sems,
):
    rest = pltpu.make_async_copy(grad_in, grad_pre, side_sems.at[0])
    rest.start()
    index = pltpu.make_async_copy(target_in, target, side_sems.at[1])
    index.start()
    rows, slots, block, _ = tiles.shape
    loads = started(adjacency, tiles, load_sems, range(0, rows, GROUP))
    sums[...] = jnp.zeros(sums.shape, F32)
    rest.wait()
    grad_agg = lax.dot_general(
        weight[...], grad_pre[...], (((1,), (1,)), ((), ())), preferred_element_type=F32
    ).astype(BF16)
    index.wait()
    for r in range(rows):
        if r in loads:
            loads[r].wait()
        spread = jnp.dot(
            grad_agg[:, r * block : (r + 1) * block],
            jnp.concatenate([tiles[r, k] for k in range(slots)], axis=1),
            preferred_element_type=F32,
        )
        for k in range(slots):
            sums[target[r * slots + k]] += spread[:, k * block : (k + 1) * block]
    for c in range(rows):
        input_grad[pl.ds(c * block, block), :] = sums[c].T.astype(BF16)


def packed(total):
    tail = total[total.shape[0] - SPARE :]
    rest = tail - tail.astype(BF16).astype(F32)
    return jnp.concatenate([total, rest], axis=0).astype(BF16)


def unpacked(values):
    wide = values.astype(F32)
    end = wide.shape[0] - SPARE
    return jnp.concatenate([wide[: end - SPARE], wide[end - SPARE : end] + wide[end:]], axis=0)


def pair_kernel(a, b, out):
    out[...] = packed(a[...] + b[...])


def sum_of_four(a, b, c, d):
    return (unpacked(a[...]) + unpacked(c[...])) + (unpacked(b[...]) + unpacked(d[...]))


def four_kernel(a, b, c, d, out):
    out[...] = packed(sum_of_four(a, b, c, d))


def copies_kernel(a, b, c, d, out):
    values = packed(sum_of_four(a, b, c, d))
    for i in range(out.shape[0]):
        out[i] = values


def last_kernel(scale, copies, weight_grad, bias_grad):
    total = copies[0].astype(F32)
    for i in range(1, copies.shape[0]):
        total += copies[i].astype(F32)
    features = weight_grad.shape[0]
    weight_grad[...] = total[:features] * scale
    both = total[features : features + SPARE] + total[features + SPARE :]
    bias_grad[...] = both[:1] * scale


VMEM = pl.BlockSpec(memory_space=pltpu.VMEM)
ANY = pl.BlockSpec(memory_space=pltpu.HBM)


def local_call(kernel, outs, *args, specs=None, out_specs=None, scratch=(), flops=0, limit=2):
    return pl.pallas_call(
        kernel,
        out_shape=outs,
        in_specs=specs or [VMEM] * len(args),
        out_specs=out_specs or [VMEM] * len(outs),
        scratch_shapes=list(scratch),
        compiler_params=pltpu.CompilerParams(vmem_limit_bytes=limit * 2**20),
        cost_estimate=pl.CostEstimate(flops=flops, bytes_accessed=0, transcendentals=0)
        if flops
        else None,
    )(*args)


def per_device(
    layer_input, history, adjacency, tile_source, counts, requests, send_ids, weight, layer_bias,
    cotangent,
):
    rows, slots, block = adjacency.shape[2:5]
    features = layer_input.shape[1]
    far, near = GRP
    far_size, near_size = lax.axis_size(far), lax.axis_size(near)
    members = lax.axis_size(MEM)
    groups = far_size * near_size
    at_far, at_near = lax.axis_index(far), lax.axis_index(near)
    blocks = history.reshape(rows, block, features)

    asked = requests[0, 0].reshape(1, 1, -1)
    asked = exchanged(jnp.broadcast_to(asked, (members, 1, asked.shape[2])), [member_order()])
    at_member = lax.axis_index(MEM)
    mine = jnp.arange(asked.shape[2], dtype=jnp.int32) == at_member
    wanted = jnp.sum(jnp.where(mine[None, None, :], asked, 0), axis=(1, 2))

    each = send_ids.shape[-1]
    ids = send_ids[0, 0].reshape(far_size, near_size, each)
    far_order = (at_far + jnp.arange(far_size, dtype=jnp.int32)) % far_size
    near_order = (at_near + jnp.arange(near_size, dtype=jnp.int32)) % near_size
    order = (far_order[:, None] * near_size + near_order[None, :]).reshape(-1)
    ids = ids.reshape(groups, each).at[order].get(mode="promise_in_bounds")
    outgoing = blocks.at[ids.reshape(-1)].get(mode="promise_in_bounds")
    outgoing = outgoing.reshape(far_size, near_size * each, block, features)
    arrived = [outgoing[0]] + [shifted(outgoing[by], far, by) for by in range(1, far_size)]
    border_a = jnp.concatenate([a[:each] for a in arrived], axis=0)
    border_b = shifted(jnp.concatenate([a[each:] for a in arrived], axis=0), near, 1)

    served = blocks.at[wanted.reshape(-1)].get(mode="promise_in_bounds")
    fetched = exchanged(served, [member_order()])

    source = tile_source[0, 0].reshape(-1)
    first_border = rows + members
    group = (source - first_border) // each
    side = (group % near_size != at_near).astype(jnp.int32)
    hop = (at_far - group // near_size) % far_size
    moved = first_border + side * (far_size * each) + hop * each + (source - first_border) % each
    member = source - rows
    turned = (member // NEAR_Z - TURN_Y) % NEAR_Y * NEAR_Z + (member - TURN_Z) % NEAR_Z
    inner = jnp.where(source < rows, source, rows + turned)
    place = jnp.where(source < first_border, inner, moved)
    live = (
        jnp.arange(slots, dtype=jnp.int32)[None, :] < counts[0, 0][:, None]
    ).reshape(-1)
    sources = rows + members + groups * each
    place = jnp.where(live, place, sources)
    target = jnp.where(live & (source < rows), source, rows)

    nodes = rows * block
    tiles = pltpu.with_memory_space_constraint(adjacency[0, 0], pltpu.HBM)
    whole = jax.ShapeDtypeStruct((nodes, features), BF16)
    stored = pltpu.HBM((nodes, features), BF16)
    term_shape = jax.ShapeDtypeStruct((features + SPARE, features), F32)
    head = pltpu.with_memory_space_constraint(adjacency[0, 0, :HEAD], pltpu.VMEM)
    loaded = pltpu.VMEM(tiles.shape, BF16)
    table_of = pltpu.SMEM((rows * slots,), jnp.int32)
    load_sems = pltpu.SemaphoreType.DMA((rows,))
    layer_output, grad_pre, term = local_call(
        forward_kernel,
        [stored, stored, term_shape],
        place, tiles, head, layer_input.reshape(rows, block, features), fetched, border_a, border_b,
        weight, layer_bias.reshape(1, features),
        pltpu.with_memory_space_constraint(cotangent, pltpu.HBM),
        specs=[ANY, ANY] + [VMEM] * 7 + [ANY],
        out_specs=[ANY, ANY, VMEM],
        scratch=[
            table_of,
            loaded,
            pltpu.VMEM((sources, block, features), BF16),
            *(pltpu.VMEM((nodes, features), BF16) for _ in range(4)),
            load_sems,
            pltpu.SemaphoreType.DMA((2,)),
            pltpu.SemaphoreType.DMA((CHUNKS, 2)),
        ],
        limit=24,
    )
    sent = jax.ShapeDtypeStruct((features + 2 * SPARE, features), BF16)
    (total,) = local_call(pair_kernel, [sent], term, shifted(term, near, 1))
    (total,) = local_call(four_kernel, [sent], *all_four(total, far))
    depth = NEAR_Z
    (copies,) = local_call(
        copies_kernel,
        [jax.ShapeDtypeStruct((depth, features + 2 * SPARE, features), BF16)],
        *all_four(total, MEM, NEAR_Z),
    )
    lines = [
        [y * NEAR_Z + (z + TURN_LAST) % NEAR_Z for z in range(NEAR_Z)] for y in range(NEAR_Y)
    ]
    copies = exchanged(copies, lines)
    (input_grad,) = local_call(
        backward_kernel,
        [whole],
        target, tiles, pltpu.with_memory_space_constraint(grad_pre, pltpu.HBM), weight,
        specs=[ANY, ANY, ANY, VMEM],
        scratch=[
            table_of,
            loaded,
            pltpu.VMEM((nodes, features), BF16),
            pltpu.VMEM((rows + 1, block, features), F32),
            load_sems,
            pltpu.SemaphoreType.DMA((2,)),
        ],
        flops=2 * rows * slots * block * block * features,
        limit=24,
    )
    scale = (nodes * groups * members) ** (-0.5)
    weight_grad, bias_grad = local_call(
        functools.partial(last_kernel, scale),
        [
            jax.ShapeDtypeStruct((features, features), F32),
            jax.ShapeDtypeStruct((1, features), F32),
        ],
        copies,
    )
    return layer_output, input_grad, weight_grad, bias_grad.reshape(features)


def solution(mesh):
    finer = Mesh(mesh.devices.reshape(4, 2, NEAR_Y * NEAR_Z), GRP_MEM)
    placed = (
        P(GRP_MEM, None),
        P(GRP_MEM, None),
        P(GRP, MEM, None, None, None, None),
        P(GRP, MEM, None, None),
        P(GRP, MEM, None),
        P(GRP, MEM, None, None),
        P(GRP, MEM, None, None),
        P(),
        P(),
        P(GRP_MEM, None),
    )
    return jax.shard_map(
        per_device,
        mesh=finer,
        in_specs=placed,
        out_specs=(P(GRP_MEM, None), P(GRP_MEM, None), P(), P()),
        check_vma=False,
    )
```

```python
import functools

import jax
import jax.numpy as jnp
from jax import lax
from jax.experimental import pallas as pl
from jax.experimental.pallas import tpu as pltpu
from jax.sharding import Mesh
from jax.sharding import PartitionSpec as P

MEM = "mem"
GRP = ("grp_0", "grp_1")
GRP_MEM = ("grp_0", "grp_1", "mem")
NEAR_Y, NEAR_Z = 4, 8
TURN_Y, TURN_Z = 2, 4
TURN_LAST = 4
F32 = jnp.float32
BF16 = jnp.bfloat16
CHUNKS = 2
ROOT = 0.7978845608028654
CUBIC = 0.044715
SPARE = 8
GROUP = 7
HEAD = 3
ALWAYS_LIVE = 3


def shifted(values, axis, by):
    size = lax.axis_size(axis)
    return lax.ppermute(values, axis, [(i, (i + by) % size) for i in range(size)])


def partner(values, axis, size, step, flip):
    def other(i):
        at = i // step % size
        return i + ((at ^ flip) - at) * step

    return lax.ppermute(values, axis, [(i, other(i)) for i in range(lax.axis_size(axis))])


def all_four(values, axis, step=1):
    return (values, *(partner(values, axis, 4, step, flip) for flip in (1, 2, 3)))


def member_order():
    return [
        (y + TURN_Y) % NEAR_Y * NEAR_Z + (z + TURN_Z) % NEAR_Z
        for y in range(NEAR_Y)
        for z in range(NEAR_Z)
    ]


def exchanged(values, groups):
    return lax.all_to_all(values, MEM, 0, 0, axis_index_groups=groups, tiled=True)


def started(source, target, sems, firsts):
    loads = {}
    for i, r in enumerate(firsts):
        part = pl.ds(r, min(GROUP, source.shape[0] - r))
        loads[r] = pltpu.make_async_copy(source.at[part], target.at[part], sems.at[i])
        loads[r].start()
    return loads


def forward_kernel(
    place_in, adjacency, head, local, fetched, border_a, border_b, weight, bias, cotangent,
    output, grad_pre, term,
    place, tiles, table, aggregate, cotangents, out_rows, grad_rows, load_sems, side_sems,
    store_sems,
):
    index = pltpu.make_async_copy(place_in, place, side_sems.at[0])
    index.start()
    rows, slots, block, features = tiles.shape
    sources = table.shape[0]
    ready = head.shape[0]
    loads = started(adjacency, tiles, load_sems, range(ready, rows, GROUP))
    side = pltpu.make_async_copy(cotangent, cotangents, side_sems.at[1])
    side.start()
    first = 0
    for part in (local, fetched, border_a, border_b):
        table[pl.ds(first, part.shape[0])] = part[...]
        first += part.shape[0]
    index.wait()
    for r in range(rows):
        if r in loads:
            loads[r].wait()
        left, right = [], []
        for k in range(slots):
            at = place[r * slots + k]
            tile = head[r, k] if r < ready else tiles[r, k]
            if k >= ALWAYS_LIVE:
                tile = jnp.where(at < sources, tile, jnp.zeros_like(tile))
            left.append(tile)
            right.append(table[at % sources])
        total = jnp.dot(
            jnp.concatenate(left, axis=1),
            jnp.concatenate(right, axis=0),
            preferred_element_type=F32,
        )
        aggregate[pl.ds(r * block, block), :] = total.astype(BF16)
    side.wait()
    lines = rows * block // CHUNKS
    weight_term = jnp.zeros((features, features), F32)
    bias_term = jnp.zeros((1, features), F32)
    stores = []
    for i in range(CHUNKS):
        at = pl.ds(i * lines, lines)
        agg = aggregate[at, :]
        v = jnp.dot(agg, weight[...], preferred_element_type=F32) + bias[...]
        square = v * v
        t = jnp.tanh(ROOT * (v * (1.0 + CUBIC * square)))
        half = 0.5 * (1.0 + t)
        out_rows[at, :] = (v * half).astype(BF16)
        slope = half + (0.5 * ROOT) * v * (1.0 - t * t) * (1.0 + (3.0 * CUBIC) * square)
        grad = (cotangents[at, :].astype(F32) * slope).astype(BF16)
        grad_rows[at, :] = grad
        for j, (here, there) in enumerate(((out_rows, output), (grad_rows, grad_pre))):
            store = pltpu.make_async_copy(here.at[at, :], there.at[at, :], store_sems.at[i, j])
            store.start()
            stores.append(store)
        weight_term += lax.dot_general(
            agg, grad, (((0,), (0,)), ((), ())), preferred_element_type=F32
        )
        bias_term += jnp.sum(grad.astype(F32), axis=0, keepdims=True)
    term[pl.ds(0, features), :] = weight_term
    term[pl.ds(features, SPARE), :] = jnp.broadcast_to(bias_term, (SPARE, features))
    for store in stores:
        store.wait()


def backward_kernel(
    target_in, adjacency, grad_in, weight, input_grad,
    target, tiles, grad_pre, sums, load_sems, side_sems,
):
    rest = pltpu.make_async_copy(grad_in, grad_pre, side_sems.at[0])
    rest.start()
    index = pltpu.make_async_copy(target_in, target, side_sems.at[1])
    index.start()
    rows, slots, block, _ = tiles.shape
    loads = started(adjacency, tiles, load_sems, range(0, rows, GROUP))
    sums[...] = jnp.zeros(sums.shape, F32)
    rest.wait()
    grad_agg = lax.dot_general(
        weight[...], grad_pre[...], (((1,), (1,)), ((), ())), preferred_element_type=F32
    ).astype(BF16)
    index.wait()
    for r in range(rows):
        if r in loads:
            loads[r].wait()
        spread = jnp.dot(
            grad_agg[:, r * block : (r + 1) * block],
            jnp.concatenate([tiles[r, k] for k in range(slots)], axis=1),
            preferred_element_type=F32,
        )
        for k in range(slots):
            sums[target[r * slots + k]] += spread[:, k * block : (k + 1) * block]
    for c in range(rows):
        input_grad[pl.ds(c * block, block), :] = sums[c].T.astype(BF16)


def packed(total):
    tail = total[total.shape[0] - SPARE :]
    rest = tail - tail.astype(BF16).astype(F32)
    return jnp.concatenate([total, rest], axis=0).astype(BF16)


def unpacked(values):
    wide = values.astype(F32)
    end = wide.shape[0] - SPARE
    return jnp.concatenate([wide[: end - SPARE], wide[end - SPARE : end] + wide[end:]], axis=0)


def pair_kernel(a, b, out):
    out[...] = packed(a[...] + b[...])


def sum_of_four(a, b, c, d):
    return (unpacked(a[...]) + unpacked(c[...])) + (unpacked(b[...]) + unpacked(d[...]))


def four_kernel(a, b, c, d, out):
    out[...] = packed(sum_of_four(a, b, c, d))


def copies_kernel(a, b, c, d, out):
    values = packed(sum_of_four(a, b, c, d))
    for i in range(out.shape[0]):
        out[i] = values


def last_kernel(scale, copies, weight_grad, bias_grad):
    total = copies[0].astype(F32)
    for i in range(1, copies.shape[0]):
        total += copies[i].astype(F32)
    features = weight_grad.shape[0]
    weight_grad[...] = total[:features] * scale
    both = total[features : features + SPARE] + total[features + SPARE :]
    bias_grad[...] = both[:1] * scale


VMEM = pl.BlockSpec(memory_space=pltpu.VMEM)
ANY = pl.BlockSpec(memory_space=pltpu.HBM)


def local_call(kernel, outs, *args, specs=None, out_specs=None, scratch=(), flops=0, limit=2):
    return pl.pallas_call(
        kernel,
        out_shape=outs,
        in_specs=specs or [VMEM] * len(args),
        out_specs=out_specs or [VMEM] * len(outs),
        scratch_shapes=list(scratch),
        compiler_params=pltpu.CompilerParams(vmem_limit_bytes=limit * 2**20),
        cost_estimate=pl.CostEstimate(flops=flops, bytes_accessed=0, transcendentals=0)
        if flops
        else None,
    )(*args)


def per_device(
    layer_input, history, adjacency, tile_source, counts, requests, send_ids, weight, layer_bias,
    cotangent,
):
    rows, slots, block = adjacency.shape[2:5]
    features = layer_input.shape[1]
    far, near = GRP
    far_size, near_size = lax.axis_size(far), lax.axis_size(near)
    members = lax.axis_size(MEM)
    groups = far_size * near_size
    at_far, at_near = lax.axis_index(far), lax.axis_index(near)
    blocks = history.reshape(rows, block, features)

    asked = requests[0, 0].reshape(1, 1, -1)
    asked = exchanged(jnp.broadcast_to(asked, (members, 1, asked.shape[2])), [member_order()])
    at_member = lax.axis_index(MEM)
    mine = jnp.arange(asked.shape[2], dtype=jnp.int32) == at_member
    wanted = jnp.sum(jnp.where(mine[None, None, :], asked, 0), axis=(1, 2))

    each = send_ids.shape[-1]
    ids = send_ids[0, 0].reshape(far_size, near_size, each)
    far_order = (at_far + jnp.arange(far_size, dtype=jnp.int32)) % far_size
    near_order = (at_near + jnp.arange(near_size, dtype=jnp.int32)) % near_size
    order = (far_order[:, None] * near_size + near_order[None, :]).reshape(-1)
    ids = ids.reshape(groups, each).at[order].get(mode="promise_in_bounds")
    outgoing = blocks.at[ids.reshape(-1)].get(mode="promise_in_bounds")
    outgoing = outgoing.reshape(far_size, near_size * each, block, features)
    arrived = [outgoing[0]] + [shifted(outgoing[by], far, by) for by in range(1, far_size)]
    border_a = jnp.concatenate([a[:each] for a in arrived], axis=0)
    border_b = shifted(jnp.concatenate([a[each:] for a in arrived], axis=0), near, 1)

    served = blocks.at[wanted.reshape(-1)].get(mode="promise_in_bounds")
    fetched = exchanged(served, [member_order()])

    source = tile_source[0, 0].reshape(-1)
    first_border = rows + members
    group = (source - first_border) // each
    side = (group % near_size != at_near).astype(jnp.int32)
    hop = (at_far - group // near_size) % far_size
    moved = first_border + side * (far_size * each) + hop * each + (source - first_border) % each
    member = source - rows
    turned = (member // NEAR_Z - TURN_Y) % NEAR_Y * NEAR_Z + (member - TURN_Z) % NEAR_Z
    inner = jnp.where(source < rows, source, rows + turned)
    place = jnp.where(source < first_border, inner, moved)
    live = (
        jnp.arange(slots, dtype=jnp.int32)[None, :] < counts[0, 0][:, None]
    ).reshape(-1)
    sources = rows + members + groups * each
    place = jnp.where(live, place, sources)
    target = jnp.where(live & (source < rows), source, rows)

    nodes = rows * block
    tiles = pltpu.with_memory_space_constraint(adjacency[0, 0], pltpu.HBM)
    whole = jax.ShapeDtypeStruct((nodes, features), BF16)
    stored = pltpu.HBM((nodes, features), BF16)
    term_shape = jax.ShapeDtypeStruct((features + SPARE, features), F32)
    head = pltpu.with_memory_space_constraint(adjacency[0, 0, :HEAD], pltpu.VMEM)
    loaded = pltpu.VMEM(tiles.shape, BF16)
    table_of = pltpu.SMEM((rows * slots,), jnp.int32)
    load_sems = pltpu.SemaphoreType.DMA((rows,))
    layer_output, grad_pre, term = local_call(
        forward_kernel,
        [stored, stored, term_shape],
        place, tiles, head, layer_input.reshape(rows, block, features), fetched, border_a, border_b,
        weight, layer_bias.reshape(1, features),
        pltpu.with_memory_space_constraint(cotangent, pltpu.HBM),
        specs=[ANY, ANY] + [VMEM] * 7 + [ANY],
        out_specs=[ANY, ANY, VMEM],
        scratch=[
            table_of,
            loaded,
            pltpu.VMEM((sources, block, features), BF16),
            *(pltpu.VMEM((nodes, features), BF16) for _ in range(4)),
            load_sems,
            pltpu.SemaphoreType.DMA((2,)),
            pltpu.SemaphoreType.DMA((CHUNKS, 2)),
        ],
        limit=24,
    )
    sent = jax.ShapeDtypeStruct((features + 2 * SPARE, features), BF16)
    (total,) = local_call(pair_kernel, [sent], term, shifted(term, near, 1))
    (total,) = local_call(four_kernel, [sent], *all_four(total, far))
    depth = NEAR_Z
    (copies,) = local_call(
        copies_kernel,
        [jax.ShapeDtypeStruct((depth, features + 2 * SPARE, features), BF16)],
        *all_four(total, MEM, NEAR_Z),
    )
    lines = [
        [y * NEAR_Z + (z + TURN_LAST) % NEAR_Z for z in range(NEAR_Z)] for y in range(NEAR_Y)
    ]
    copies = exchanged(copies, lines)
    (input_grad,) = local_call(
        backward_kernel,
        [whole],
        target, tiles, pltpu.with_memory_space_constraint(grad_pre, pltpu.HBM), weight,
        specs=[ANY, ANY, ANY, VMEM],
        scratch=[
            table_of,
            loaded,
            pltpu.VMEM((nodes, features), BF16),
            pltpu.VMEM((rows + 1, block, features), F32),
            load_sems,
            pltpu.SemaphoreType.DMA((2,)),
        ],
        flops=2 * rows * slots * block * block * features,
        limit=24,
    )
    scale = (nodes * groups * members) ** (-0.5)
    weight_grad, bias_grad = local_call(
        functools.partial(last_kernel, scale),
        [
            jax.ShapeDtypeStruct((features, features), F32),
            jax.ShapeDtypeStruct((1, features), F32),
        ],
        copies,
    )
    return layer_output, input_grad, weight_grad, bias_grad.reshape(features)


def solution(mesh):
    finer = Mesh(mesh.devices.reshape(4, 2, NEAR_Y * NEAR_Z), GRP_MEM)
    placed = (
        P(GRP_MEM, None),
        P(GRP_MEM, None),
        P(GRP, MEM, None, None, None, None),
        P(GRP, MEM, None, None),
        P(GRP, MEM, None),
        P(GRP, MEM, None, None),
        P(GRP, MEM, None, None),
        P(),
        P(),
        P(GRP_MEM, None),
    )
    return jax.shard_map(
        per_device,
        mesh=finer,
        in_specs=placed,
        out_specs=(P(GRP_MEM, None), P(GRP_MEM, None), P(), P()),
        check_vma=False,
    )
```
